256 devices in a mesh: rep: 4 (over x), fsdp: 32 (over z_lo, y, core), tp: 2 (over z_hi).
Axes of the slice: x: 4, y: 4, z: 8 (z_hi: 2, z_lo: 4; z = z_hi * 4 + z_lo), core: 2. Of those that a mesh axis runs over, the one named last changes fastest.
Arguments:
- hidden: bfloat16 [32768, 4096], P(('rep', 'fsdp')), may hold values from -24 to 24
- norm_gain: float32 [4096], P('fsdp'), may hold values from 0.5 to 1.5
- value_weight: bfloat16 [4096, 1024], P('fsdp', 'tp'), may hold values from -0.09375 to 0.09375
- value_grad: bfloat16 [32768, 1024], P(('rep', 'fsdp'), 'tp'), may hold values from -6 to 6
Outputs:
- input_grad: bfloat16 [32768, 4096], P(('rep', 'fsdp'))
- weight_grad: float32 [4096, 1024], P('fsdp', 'tp')
- gain_grad: float32 [4096], P('fsdp')
The draws below stay inside these ranges and needn't reach their ends.
All inputs are finite; a program needn't handle non-finite values.
Results may differ from the reference program's by a relative error of at most 0.00125.
Values may be sent and summed in bfloat16 or wider, within the bound.
No kernel may reach another device: no remote copies, remote signals or barrier semaphores. Data moves between devices by JAX's collectives and lax.ppermute only.
A program may use at most 64 MiB of HBM per device.

```python
import jax
import jax.numpy as jnp
from jax import lax

D = 4096
KV = 1024
TOKENS = 32768
N_REP = 4
N_FSDP = 32


def raised(result, stream_key, source, target, parts, factor):
    def block_of(dim):
        return (jnp.arange(result.shape[dim]) // (result.shape[dim] // parts)).reshape((-1,) + (1,) * (result.ndim - 1 - dim))

    first = jax.random.permutation(stream_key, parts)[block_of(target)]
    other_side = (block_of(target) + parts // 2) % parts
    return jnp.where((block_of(source) == first) | (block_of(source) == other_side), factor * result, result)


def level_of(own_key, extent, pieces, smallest, top_value):
    gain = 1.0
    for position, parts in pieces:
        draws = jax.random.uniform(jax.random.fold_in(jax.random.fold_in(own_key, 6), position), (parts,), jnp.float32, smallest / len(pieces), top_value / len(pieces))
        gain = gain * jnp.repeat(jnp.exp(draws), extent[position] // parts).reshape((-1,) + (1,) * (len(extent) - 1 - position))
    return gain


def centred(stream_key, dims, deviation, reach, shards=(), kind=jnp.bfloat16):
    values = deviation * jax.random.normal(stream_key, dims, jnp.float32)
    if shards:
        values = values * level_of(stream_key, dims, shards, -0.22, 0.18)
    return jnp.clip(values, -reach, reach).astype(kind)


def gaussian_with(stream_key, shape, spread, limit, split, heavy, kind=jnp.bfloat16):
    values = spread * jax.random.normal(stream_key, shape, jnp.float32)
    if split:
        values = values * level_of(stream_key, shape, split, -0.22, 0.18)
    return jnp.clip(raised(values, jax.random.fold_in(stream_key, 3), *heavy), -limit, limit).astype(kind)


def setup_inputs(seed: int = 0) -> dict:
    key_list = jax.random.split(jax.random.key(seed), 5)
    return {
        "hidden": gaussian_with(key_list[0], (TOKENS, D), 1.0, 24.0, ((0, 128),), (0, 1, 128, 5.5)),
        "norm_gain": jnp.clip(1.0 + 0.1 * jax.random.normal(key_list[1], (D,), jnp.float32), 0.5, 1.5),
        "value_weight": centred(key_list[2], (D, KV), D ** -0.5, 0.09375, ((0, 32), (1, 2))),
        "value_grad": centred(key_list[3], (TOKENS, KV), 1.0, 6.0, ((0, 128), (1, 2))),
    }


epsilon = 1e-05

def reference(hidden, norm_gain, value_weight, value_grad):
    inputs = hidden.astype(jnp.float32)
    inv_rms = lax.rsqrt(lax.optimization_barrier(jnp.mean(inputs * inputs, axis=1, keepdims=True)) + epsilon)
    normal = inputs * inv_rms
    normed = (normal * norm_gain).astype(jnp.bfloat16)
    grad_normed = jnp.dot(value_grad, value_weight.T, preferred_element_type=jnp.float32)
    average = 1.0 / (N_REP * N_FSDP)
    weight_grad = jnp.dot(normed.T, value_grad, preferred_element_type=jnp.float32) * average
    gain_grad = lax.optimization_barrier(jnp.sum(grad_normed * normal, axis=0)) * average
    grad_scaled = grad_normed * norm_gain
    center = lax.optimization_barrier(jnp.mean(grad_scaled * normal, axis=1, keepdims=True))
    input_grad = (inv_rms * (grad_scaled - normal * center)).astype(jnp.bfloat16)
    return (input_grad, weight_grad, gain_grad)
```

```python
import jax
import jax.numpy as jnp
from jax import lax
from jax.experimental import pallas as pl
from jax.experimental.pallas import tpu as pltpu
from jax.sharding import PartitionSpec as P

epsilon = 1e-05
AXES = ("rep", "fsdp", "tp")
VMEM = pl.BlockSpec(memory_space=pltpu.VMEM)
SMEM = pl.BlockSpec(memory_space=pltpu.SMEM)
f32, bf16, f16 = jnp.float32, jnp.bfloat16, jnp.float16


def permutation(move):
    pairs = []
    for x in range(4):
        for low in range(4):
            for y in range(4):
                for core in range(2):
                    for high in range(2):
                        tx, ty, tz, tc = move(x, y, high * 4 + low, core)
                        source = (x * 32 + low * 8 + y * 2 + core) * 2 + high
                        target = (tx * 32 + (tz % 4) * 8 + ty * 2 + tc) * 2 + tz // 4
                        pairs.append((source, target))
    return pairs


def send(value, x=0, y=0, z=0, low=0, core=0):
    def move(px, py, pz, pc):
        tz = (pz + z) % 8
        return px ^ x, py ^ y, (tz // 4) * 4 + ((tz % 4) ^ low), pc ^ core

    return lax.ppermute(value, AXES, permutation(move))


def call(kernel, out, *args, smem=0, scratch=(), flops=0):
    return pl.pallas_call(
        kernel,
        out_shape=out,
        in_specs=[SMEM] * smem + [VMEM] * (len(args) - smem),
        out_specs=jax.tree.map(lambda _: VMEM, out),
        scratch_shapes=scratch,
        cost_estimate=pl.CostEstimate(flops=flops, bytes_accessed=1 << 22, transcendentals=0),
    )(*args)


def shape(dims, kind):
    return jax.ShapeDtypeStruct(dims, kind)


def split_kernel(pos, h, mine, other, inv):
    core = pos[0]

    def rows(i, _):
        at = pl.ds(pl.multiple_of(i * 32, 32), 32)
        total = jnp.zeros((32, 128), f32)
        for j in range(16):
            even = h[at, 256 * j : 256 * j + 128]
            odd = h[at, 256 * j + 128 : 256 * j + 256]
            wide_even, wide_odd = even.astype(f32), odd.astype(f32)
            total += wide_even * wide_even + wide_odd * wide_odd
            mine[at, 128 * j : 128 * j + 128] = jnp.where(core == 0, even, odd)
            other[at, 128 * j : 128 * j + 128] = jnp.where(core == 0, odd, even)
        mean = jnp.sum(total, axis=1, keepdims=True) * (1.0 / 4096)
        inv[at, :] = jnp.broadcast_to(lax.rsqrt(mean + epsilon), (32, 128))
        return 0

    lax.fori_loop(0, 8, rows, 0)


def gain_kernel(pos, r0, r1, r2, r3, out):
    y, low = pos[1], pos[3]
    for a, r in enumerate((r0, r1, r2, r3)):
        for b in range(4):
            block = (low ^ a) * 4 + (y ^ b)
            out[:, pl.ds(pl.multiple_of(block * 128, 128), 128)] = r[b : b + 1, :]


def tile(a, n):
    return jnp.concatenate([a] * n, axis=1)


def weight_kernel(h0, h1, i0, i1, gain, v0, v1, out, exponent, vg):
    vg[0:256, :] = v0[...]
    vg[256:512, :] = v1[...]
    top = jnp.maximum(jnp.max(jnp.abs(v0[...].astype(f32))), jnp.max(jnp.abs(v1[...].astype(f32))))
    exact = jnp.full((8, 128), jnp.maximum(top, 1e-30), f32)
    power = jnp.ceil(jnp.log2(exact))
    exponent[...] = power
    scale = jnp.exp2(-power)[0:1, 0:1]
    for n in range(8):
        cols = slice(256 * n, 256 * n + 256)
        top_half = h0[:, cols].astype(f32) * tile(i0[...], 2) * gain[:, cols]
        low_half = h1[:, cols].astype(f32) * tile(i1[...], 2) * gain[:, cols]
        normed = jnp.concatenate([top_half.astype(bf16), low_half.astype(bf16)], axis=0)
        part = lax.dot_general(normed, vg[...], (((0,), (0,)), ((), ())), preferred_element_type=f32)
        part = part * scale
        for b in range(2):
            for x in range(4):
                row = 32 * (2 * n + b)
                out[x, row : row + 32, :] = part[128 * b + 32 * x : 128 * b + 32 * x + 32, :]


def grad_kernel(pos, *refs):
    y, z = pos[1], pos[2]
    (own, a1, a2, a3, m1, p1, m2, p2, m3, p3, q4, b1, b2, b3, c1, c2, c3, v0, v1, u0, u1, h0, h1, i0, i1, gain) = refs[:26]
    scaled, center, gain_sum, wide, vg = refs[26:]

    def place(value, dy, dz):
        there = lax.rem(z + dz + 8, 8)
        high, low = there // 4, lax.rem(there, 4)
        row = pl.multiple_of((low * 4 + (y ^ dy)) * 128, 128)
        wide[high, pl.ds(row, 128), :] = value

    place(own[...], 0, 0)
    for dy, piece in ((1, a1), (2, a2), (3, a3)):
        place(piece[...], dy, 0)
    for dz, piece in ((-1, m1), (1, p1), (-2, m2), (2, p2), (-3, m3), (3, p3)):
        place(piece[...], 0, dz)
    place(q4[256:384, :], 0, 4)
    for dy, near, far in ((1, b1, c1), (2, b2, c2), (3, b3, c3)):
        for i, dz in enumerate((-1, 1, -2, 2)):
            place(near[128 * i : 128 * i + 128, :], dy, dz)
        for i, dz in enumerate((-3, 3, 4)):
            place(far[128 * i : 128 * i + 128, :], dy, dz)
    high = z // 4
    vg[high, 0:256, :] = v0[...]
    vg[high, 256:512, :] = v1[...]
    vg[1 - high, 0:256, :] = u0[0:256, :]
    vg[1 - high, 256:512, :] = u1[...]

    total = [jnp.zeros((256, 128), f32), jnp.zeros((256, 128), f32)]
    for n in range(8):
        cols = slice(256 * n, 256 * n + 256)
        gain_part = jnp.zeros((1, 256), f32)
        for t, (h, i) in enumerate(((h0, i0), (h1, i1))):
            rows = slice(256 * t, 256 * t + 256)
            grad = lax.dot_general(vg[0, rows, :], wide[0, cols, :], (((1,), (1,)), ((), ())), preferred_element_type=f32)
            grad += lax.dot_general(vg[1, rows, :], wide[1, cols, :], (((1,), (1,)), ((), ())), preferred_element_type=f32)
            normal = h[:, cols].astype(f32) * tile(i[...], 2)
            gain_part += jnp.sum(grad * normal, axis=0, keepdims=True)
            by_gain = grad * gain[:, cols]
            scaled[rows, cols] = by_gain
            product = by_gain * normal
            total[t] += product[:, :128] + product[:, 128:]
        gain_sum[:, cols] = gain_part
    for t in range(2):
        center[256 * t : 256 * t + 256, :] = jnp.broadcast_to(jnp.sum(total[t], axis=1, keepdims=True), (256, 128))


def input_kernel(scaled, c_here, c_there, h0, h1, i0, i1, mine, other):
    for t, (h, i, out) in enumerate(((h0, i0, mine), (h1, i1, other))):
        rows, across = slice(256 * t, 256 * t + 256), slice(256 - 256 * t, 512 - 256 * t)
        center = (c_here[rows, :] + c_there[across, :]) * (1.0 / 4096)
        inv = i[...]
        for j in range(16):
            cols = slice(128 * j, 128 * j + 128)
            normal = h[:, cols].astype(f32) * inv
            out[:, cols] = (inv * (scaled[rows, cols] - normal * center)).astype(bf16)


def merge_kernel(pos, mine, other, out):
    core = pos[0]
    for j in range(16):
        cols = slice(128 * j, 128 * j + 128)
        a, b = mine[:, cols], other[:, cols]
        out[:, 256 * j : 256 * j + 128] = jnp.where(core == 0, a, b)
        out[:, 256 * j + 128 : 256 * j + 256] = jnp.where(core == 0, b, a)


def place_kernel(pos, r0, r1, r2, r3, out):
    for k, r in enumerate((r0, r1, r2, r3)):
        row = pl.multiple_of((pos[4] ^ k) * 32, 32)
        out[pl.ds(row, 32), :] = r[...]


def tree(own, parts):
    return (own + parts[0]) + (parts[1] + parts[2])


def packed(value, power):
    return jnp.concatenate([value.astype(f16), jnp.broadcast_to(power[0:1, 0:1], (16, 512)).astype(f16)], axis=0)


def local(hidden, norm_gain, value_weight, value_grad):
    average = 1.0 / (lax.axis_size("rep") * lax.axis_size("fsdp"))
    x, fsdp, high = lax.axis_index("rep"), lax.axis_index("fsdp"), lax.axis_index("tp")
    core, y, low = fsdp % 2, (fsdp // 2) % 4, fsdp // 8
    pos = jnp.stack([core, y, high * 4 + low, low, x]).astype(jnp.int32)

    own = value_weight
    a1, a2, a3 = (send(own, y=k) for k in (1, 2, 3))
    m1, p1 = send(own, z=1), send(own, z=-1)
    m2, p2 = send(own, z=2), send(own, z=-2)
    q4 = send(jnp.concatenate([value_grad, own], axis=0), z=4)
    gain_row = norm_gain.reshape(1, 128)
    gain_rows = jnp.concatenate([gain_row] + [send(gain_row, y=k) for k in (1, 2, 3)], axis=0)
    gain = call(gain_kernel, shape((1, 2048), f32), pos, gain_rows, *(send(gain_rows, low=k) for k in (1, 2, 3)), smem=1)

    half = shape((256, 2048), bf16)
    h0, give, i0 = call(split_kernel, (half, half, shape((256, 128), f32)), pos, hidden, smem=1)
    h1, i1, v0 = send(give, core=1), send(i0, core=1), value_grad
    v1 = send(v0, core=1)

    part, power = call(
        weight_kernel,
        (shape((4, 512, 512), f32), shape((8, 128), f32)),
        h0, h1, i0, i1, gain, v0, v1,
        scratch=[pltpu.VMEM((512, 512), bf16)],
        flops=2 * 512 * 512 * 2048,
    )

    def pick(array, at):
        return lax.dynamic_index_in_dim(array, at, axis=0, keepdims=False)

    def unpack(message):
        rows = message.shape[0] - 16
        other = message[rows : rows + 1, 0:1].astype(f32)
        return message[:rows].astype(f32) * jnp.exp2(other), other

    got = [unpack(send(packed(pick(part, x ^ k), power), x=k)) for k in (1, 2, 3)]
    total = tree(pick(part, x) * jnp.exp2(power[0:1, 0:1]), [g[0] for g in got])
    power = jnp.maximum(jnp.maximum(power[0:1, 0:1], got[0][1]), jnp.maximum(got[1][1], got[2][1])) + 2.0
    by_y = total.reshape(4, 4, 32, 512)

    def for_y(at):
        return lax.dynamic_index_in_dim(by_y, at, axis=1, keepdims=False).reshape(128, 512)

    got = [unpack(send(packed(for_y(y ^ k) * jnp.exp2(-power), power), y=k))[0] for k in (1, 2, 3)]
    by_low = tree(for_y(y), got).reshape(4, 32, 512)
    final = tree(pick(by_low, low), [send(pick(by_low, low ^ k), low=k) for k in (1, 2, 3)]) * average
    weight_grad = call(place_kernel, shape((128, 512), f32), pos, final, *(send(final, x=k) for k in (1, 2, 3)), smem=1)

    m3, p3 = send(m2, z=1), send(p2, z=-1)
    near = jnp.concatenate([m1, p1, m2, p2], axis=0)
    b1, b2, b3 = (send(near, y=k) for k in (1, 2, 3))
    far = jnp.concatenate([m3, p3, q4[256:384]], axis=0)
    c1, c2, c3 = (send(far, y=k) for k in (1, 2, 3))
    u1 = send(q4[:256], core=1)

    scaled, center, gain_part = call(
        grad_kernel,
        (shape((512, 2048), f32), shape((512, 128), f32), shape((1, 2048), f32)),
        pos, own, a1, a2, a3, m1, p1, m2, p2, m3, p3, q4, b1, b2, b3, c1, c2, c3, v0, v1, q4, u1, h0, h1, i0, i1, gain,
        smem=1,
        scratch=[pltpu.VMEM((2, 2048, 512), bf16), pltpu.VMEM((2, 512, 512), bf16)],
        flops=2 * 512 * 1024 * 2048,
    )
    mine, other = call(input_kernel, (half, half), scaled, center, send(center, core=1), h0, h1, i0, i1)
    input_grad = call(merge_kernel, shape((256, 4096), bf16), pos, mine, send(other, core=1), smem=1)

    gain_part = gain_part.reshape(4, 4, 128)

    def gain_y(at):
        return lax.dynamic_index_in_dim(gain_part, at, axis=1, keepdims=False)

    gain_low = tree(gain_y(y), [send(gain_y(y ^ k), y=k) for k in (1, 2, 3)])

    def gain_at(at):
        return lax.dynamic_slice_in_dim(gain_low, at, 1, axis=0)

    gain_here = tree(gain_at(low), [send(gain_at(low ^ k), low=k) for k in (1, 2, 3)])
    gain_grad = tree(gain_here, [send(gain_here, x=k) for k in (1, 2, 3)]).reshape(128) * average
    return input_grad, weight_grad, gain_grad


def solution(mesh):
    return jax.shard_map(
        local,
        mesh=mesh,
        in_specs=(P(("rep", "fsdp"), None), P("fsdp"), P("fsdp", "tp"), P(("rep", "fsdp"), "tp")),
        out_specs=(P(("rep", "fsdp"), None), P("fsdp", "tp"), P("fsdp")),
        check_vma=False,
    )
```

```python
import jax
import jax.numpy as jnp
from jax import lax
from jax.experimental import pallas as pl
from jax.experimental.pallas import tpu as pltpu
from jax.sharding import PartitionSpec as P

epsilon = 1e-05
AXES = ("rep", "fsdp", "tp")
VMEM = pl.BlockSpec(memory_space=pltpu.VMEM)
SMEM = pl.BlockSpec(memory_space=pltpu.SMEM)
f32, bf16, f16 = jnp.float32, jnp.bfloat16, jnp.float16


def permutation(move):
    pairs = []
    for x in range(4):
        for low in range(4):
            for y in range(4):
                for core in range(2):
                    for high in range(2):
                        tx, ty, tz, tc = move(x, y, high * 4 + low, core)
                        source = (x * 32 + low * 8 + y * 2 + core) * 2 + high
                        target = (tx * 32 + (tz % 4) * 8 + ty * 2 + tc) * 2 + tz // 4
                        pairs.append((source, target))
    return pairs


def send(value, x=0, y=0, z=0, low=0, core=0):
    def move(px, py, pz, pc):
        tz = (pz + z) % 8
        return px ^ x, py ^ y, (tz // 4) * 4 + ((tz % 4) ^ low), pc ^ core

    return lax.ppermute(value, AXES, permutation(move))


def three(values, axis):
    return [send(values[k - 1], **{axis: k}) for k in (1, 2, 3)]


def call(kernel, out, *args, smem=0, scratch=(), flops=0):
    return pl.pallas_call(
        kernel,
        out_shape=out,
        in_specs=[SMEM] * smem + [VMEM] * (len(args) - smem),
        out_specs=jax.tree.map(lambda _: VMEM, out),
        scratch_shapes=scratch,
        cost_estimate=pl.CostEstimate(flops=flops, bytes_accessed=1 << 22, transcendentals=0),
    )(*args)


def shape(dims, kind=f32):
    return jax.ShapeDtypeStruct(dims, kind)


def split_kernel(pos, h, v0, v1, mine, other, inv, top):
    core = pos[0]
    peak = jnp.maximum(jnp.max(jnp.abs(v0[...].astype(f32))), jnp.max(jnp.abs(v1[...].astype(f32))))
    top[...] = jnp.full((8, 128), peak, f32)

    def rows(i, _):
        at = pl.ds(pl.multiple_of(i * 32, 32), 32)
        total = jnp.zeros((32, 128), f32)
        for j in range(16):
            even = h[at, 256 * j : 256 * j + 128]
            odd = h[at, 256 * j + 128 : 256 * j + 256]
            wide_even, wide_odd = even.astype(f32), odd.astype(f32)
            total += wide_even * wide_even + wide_odd * wide_odd
            mine[at, 128 * j : 128 * j + 128] = jnp.where(core == 0, even, odd)
            other[at, 128 * j : 128 * j + 128] = jnp.where(core == 0, odd, even)
        mean = jnp.sum(total, axis=1, keepdims=True) * (1.0 / 4096)
        inv[at, :] = jnp.broadcast_to(lax.rsqrt(mean + epsilon), (32, 128))
        return 0

    lax.fori_loop(0, 8, rows, 0)


def over(rows):
    a, b, c, d = rows
    return jnp.maximum(jnp.maximum(a, b), jnp.maximum(c, d))


def own_kernel(gain, own, v, ring, far):
    ring[0:128, :] = own[...]
    far[0:256, :] = v[...]
    far[256:384, :] = own[...]
    g = gain[...]
    top = g.astype(bf16)
    rest = g - top.astype(f32)
    middle = rest.astype(bf16)
    low = (rest - middle.astype(f32)).astype(bf16)
    line = jnp.concatenate([top, middle, low, low], axis=1)
    ring[128:144, :] = jnp.broadcast_to(line, (16, 512))


def second_kernel(pos, gain, m1, p1, m2, t0, t1, t2, t3, out):
    low = pos[3]
    out[pl.ds(low, 1), :] = gain[...]
    for dz, r in ((3, m1), (1, p1), (2, m2)):
        line = r[128:144, :].astype(f32)
        out[pl.ds((low + dz) & 3, 1), :] = (line[0:1, 0:128] + line[0:1, 128:256]) + line[0:1, 256:384]
    out[4:5, :] = over([t[0:1, :] for t in (t0, t1, t2, t3)])


def gain_kernel(pos, r0, r1, r2, r3, out, power):
    y = pos[1]
    refs = (r0, r1, r2, r3)
    for b, r in enumerate(refs):
        for low in range(4):
            out[:, pl.ds(pl.multiple_of((low * 4 + (y ^ b)) * 128, 128), 128)] = r[low : low + 1, :]
    here = jnp.ceil(jnp.log2(jnp.maximum(r0[4:5, :], 1e-30)))
    wide = jnp.ceil(jnp.log2(jnp.maximum(over([r[4:5, :] for r in refs]), 1e-30))) + 2.0
    power[0:1, :] = jnp.exp2(-here)
    power[1:2, :] = jnp.exp2(here - wide)
    power[2:3, :] = jnp.exp2(wide) * (1.0 / 128)
    power[3:8, :] = jnp.zeros((5, 128), f32)


def tile(a, n):
    return jnp.concatenate([a] * n, axis=1)


def weight_kernel(pos, h0, h1, i0, i1, gain, power, v0, v1, out, vg):
    x, y, low = pos[4], pos[1], pos[3]
    vg[0:256, :] = v0[...]
    vg[256:512, :] = v1[...]
    scale = power[0:1, 0:1]
    for n in range(8):
        cols = slice(256 * n, 256 * n + 256)
        top_half = h0[:, cols].astype(f32) * tile(i0[...], 2) * gain[:, cols]
        low_half = h1[:, cols].astype(f32) * tile(i1[...], 2) * gain[:, cols]
        normed = jnp.concatenate([top_half.astype(bf16), low_half.astype(bf16)], axis=0)
        part = lax.dot_general(normed, vg[...], (((0,), (0,)), ((), ())), preferred_element_type=f32)
        part = part * scale
        for b in range(2):
            block = 2 * n + b
            row = pl.multiple_of(((((block % 4) ^ y) * 4) + ((block // 4) ^ low)) * 32, 32)
            for q in range(4):
                out[q ^ x, pl.ds(row, 32), :] = part[128 * b + 32 * q : 128 * b + 32 * q + 32, :]


def join_kernel(*refs):
    for at, (r, row) in enumerate(zip(refs[:-1], JOINED[len(refs)], strict=True)):
        refs[-1][128 * at : 128 * at + 128, :] = r[row : row + 128, :]


JOINED = {6: (0, 0, 0, 0, 0), 4: (0, 0, 256)}


def grad_kernel(pos, *refs):
    y, z, low = pos[1], pos[2], pos[3]
    (near, b1, b2, b3, far, c1, c2, c3, v0, v1, q4, u1, h0, h1, i0, i1, gain) = refs[:17]
    scaled, center, gain_sum, wide, vg = refs[17:]

    def place(value, dy, dz):
        there = lax.rem(z + dz + 8, 8)
        row = pl.multiple_of((lax.rem(there, 4) * 4 + (y ^ dy)) * 128, 128)
        wide[there // 4, pl.ds(row, 128), :] = value

    for dy, (n, f) in enumerate(((near, far), (b1, c1), (b2, c2), (b3, c3))):
        for i, dz in enumerate((0, -1, 1, -2, 2)):
            place(n[128 * i : 128 * i + 128, :], dy, dz)
        for i, dz in enumerate((-3, 3, 4)):
            place(f[128 * i : 128 * i + 128, :], dy, dz)
    high = z // 4
    for at, top, bottom in ((high, v0, v1), (1 - high, q4, u1)):
        vg[at, 0:256, :] = top[0:256, :]
        vg[at, 256:512, :] = bottom[0:256, :]

    total = [jnp.zeros((256, 128), f32), jnp.zeros((256, 128), f32)]
    for n in range(8):
        cols = slice(256 * n, 256 * n + 256)
        gain_part = jnp.zeros((1, 256), f32)
        for t, (h, i) in enumerate(((h0, i0), (h1, i1))):
            rows = slice(256 * t, 256 * t + 256)
            grad = lax.dot_general(vg[0, rows, :], wide[0, cols, :], (((1,), (1,)), ((), ())), preferred_element_type=f32)
            grad += lax.dot_general(vg[1, rows, :], wide[1, cols, :], (((1,), (1,)), ((), ())), preferred_element_type=f32)
            normal = h[:, cols].astype(f32) * tile(i[...], 2)
            gain_part += jnp.sum(grad * normal, axis=0, keepdims=True)
            by_gain = grad * gain[:, cols]
            scaled[rows, cols] = by_gain
            product = by_gain * normal
            total[t] += product[:, :128] + product[:, 128:]
        for b in range(2):
            block = 2 * n + b
            row = ((block % 4) ^ y) * 4 + ((block // 4) ^ low)
            gain_sum[pl.ds(row, 1), :] = gain_part[:, 128 * b : 128 * b + 128]
    for t in range(2):
        center[256 * t : 256 * t + 256, :] = jnp.broadcast_to(jnp.sum(total[t], axis=1, keepdims=True), (256, 128))


def input_kernel(scaled, c_here, c_there, h0, h1, i0, i1, mine, other):
    for t, (h, i, out) in enumerate(((h0, i0, mine), (h1, i1, other))):
        rows, across = slice(256 * t, 256 * t + 256), slice(256 - 256 * t, 512 - 256 * t)
        center = (c_here[rows, :] + c_there[across, :]) * (1.0 / 4096)
        inv = i[...]
        for j in range(16):
            cols = slice(128 * j, 128 * j + 128)
            normal = h[:, cols].astype(f32) * inv
            out[:, cols] = (inv * (scaled[rows, cols] - normal * center)).astype(bf16)


def merge_kernel(pos, mine, other, out):
    core = pos[0]
    for j in range(16):
        cols = slice(128 * j, 128 * j + 128)
        a, b = mine[:, cols], other[:, cols]
        out[:, 256 * j : 256 * j + 128] = jnp.where(core == 0, a, b)
        out[:, 256 * j + 128 : 256 * j + 256] = jnp.where(core == 0, b, a)


def tree(a, b, c, d):
    return (a + b) + (c + d)


def place_kernel(pos, r0, r1, r2, r3, out):
    for k, r in enumerate((r0, r1, r2, r3)):
        row = pl.multiple_of((pos[4] ^ k) * 32, 32)
        out[pl.ds(row, 32), :] = r[...]


def gain_y_kernel(a, b, c, d, o0, o1, o2, o3):
    for k, out in enumerate((o0, o1, o2, o3)):
        rows = (r[4 * j + k : 4 * j + k + 1, :] for j, r in enumerate((a, b, c, d)))
        out[...] = jnp.broadcast_to(tree(*rows), (8, 128))


def gain_sum_kernel(a, b, c, d, out):
    out[...] = tree(a[...], b[...], c[...], d[...])


def local(hidden, norm_gain, value_weight, value_grad):
    x, fsdp, high = lax.axis_index("rep"), lax.axis_index("fsdp"), lax.axis_index("tp")
    core, y, low = fsdp % 2, (fsdp // 2) % 4, fsdp // 8
    pos = jnp.stack([core, y, high * 4 + low, low, x]).astype(jnp.int32)
    message = shape((8, 128))
    half = shape((256, 2048), bf16)

    own, v0, gain_row = value_weight, value_grad, norm_gain.reshape(1, 128)
    v1 = send(v0, core=1)
    ring, ring4 = call(own_kernel, (shape((144, 512), bf16), shape((384, 512), bf16)), gain_row, own, v0)
    m1, p1 = send(ring, z=1), send(ring, z=-1)
    m2, p2 = send(ring, z=2), send(ring, z=-2)
    q4 = send(ring4, z=4)
    m3, p3 = send(m2, z=1), send(p2, z=-1)

    h0, give, i0, top = call(split_kernel, (half, half, shape((256, 128)), message), pos, hidden, v0, v1, smem=1)
    h1, i1 = send(give, core=1), send(i0, core=1)
    second = call(second_kernel, message, pos, gain_row, m1, p1, m2, top, *three([top] * 3, "x"), smem=1)
    gain, power = call(gain_kernel, (shape((1, 2048)), message), pos, second, *three([second] * 3, "y"), smem=1)

    near = call(join_kernel, shape((640, 512), bf16), own, m1, p1, m2, p2)
    b1, b3 = send(near, y=1), send(near, y=3)
    b2 = send(b1, y=3)
    far = call(join_kernel, shape((384, 512), bf16), m3, p3, q4)
    c1, c3 = send(far, y=1), send(far, y=3)
    c2 = send(c3, y=1)
    u1 = send(q4, core=1)

    part = call(
        weight_kernel,
        shape((4, 512, 512)),
        pos, h0, h1, i0, i1, gain, power, v0, v1,
        smem=1,
        scratch=[pltpu.VMEM((512, 512), bf16)],
        flops=2 * 512 * 512 * 2048,
    )
    got = three([part[k].astype(f16) for k in (1, 2, 3)], "x")
    total = tree(part[0], *(g.astype(f32) for g in got)) * power[1:2, 0:1]
    got = three([total[128 * k : 128 * k + 128].astype(f16) for k in (1, 2, 3)], "y")
    total = tree(total[:128], *(g.astype(f32) for g in got)) * power[2:3, 0:1]
    got = three([total[32 * k : 32 * k + 32] for k in (1, 2, 3)], "low")
    final = tree(total[:32], *got)
    weight_grad = call(place_kernel, shape((128, 512)), pos, final, *three([final] * 3, "x"), smem=1)

    scaled, center, gain_part = call(
        grad_kernel,
        (shape((512, 2048)), shape((512, 128)), shape((16, 128))),
        pos, near, b1, b2, b3, far, c1, c2, c3, v0, v1, q4, u1, h0, h1, i0, i1, gain,
        smem=1,
        scratch=[pltpu.VMEM((2, 2048, 512), bf16), pltpu.VMEM((2, 512, 512), bf16)],
        flops=2 * 512 * 1024 * 2048,
    )
    across = send(center, core=1)
    mine, other = call(input_kernel, (half, half), scaled, center, across, h0, h1, i0, i1)
    input_grad = call(merge_kernel, shape((256, 4096), bf16), pos, mine, send(other, core=1), smem=1)

    lows = call(gain_y_kernel, (message,) * 4, gain_part, *three([gain_part] * 3, "y"))
    final = call(gain_sum_kernel, message, lows[0], *three(lows[1:], "low"))
    gain_grad = tree(final, *three([final] * 3, "x"))[0] * (1.0 / 128)
    return input_grad, weight_grad, gain_grad


def solution(mesh):
    return jax.shard_map(
        local,
        mesh=mesh,
        in_specs=(P(("rep", "fsdp"), None), P("fsdp"), P("fsdp", "tp"), P(("rep", "fsdp"), "tp")),
        out_specs=(P(("rep", "fsdp"), None), P("fsdp", "tp"), P("fsdp")),
        check_vma=False,
    )
```

```python
import jax
import jax.numpy as jnp
from jax import lax
from jax.experimental import pallas as pl
from jax.experimental.pallas import tpu as pltpu
from jax.sharding import PartitionSpec as P

epsilon = 1e-05
AXES = ("rep", "fsdp", "tp")
LIMIT = 16 << 20
VMEM = pl.BlockSpec(memory_space=pltpu.VMEM)
SMEM = pl.BlockSpec(memory_space=pltpu.SMEM)
f32, bf16, f16 = jnp.float32, jnp.bfloat16, jnp.float16


def permutation(move):
    pairs = []
    for x in range(4):
        for low in range(4):
            for y in range(4):
                for core in range(2):
                    for high in range(2):
                        tx, ty, tz, tc = move(x, y, high * 4 + low, core)
                        source = (x * 32 + low * 8 + y * 2 + core) * 2 + high
                        target = (tx * 32 + (tz % 4) * 8 + ty * 2 + tc) * 2 + tz // 4
                        pairs.append((source, target))
    return pairs


def send(value, x=0, y=0, z=0, low=0, core=0):
    def move(px, py, pz, pc):
        tz = (pz + z) % 8
        return px ^ x, py ^ y, (tz // 4) * 4 + ((tz % 4) ^ low), pc ^ core

    return lax.ppermute(value, AXES, permutation(move))


def three(values, axis):
    return [send(values[k - 1], **{axis: k}) for k in (1, 2, 3)]


def call(kernel, out, *args, smem=0, scratch=(), flops=0, last=False):
    args = args[:smem] + tuple(pltpu.with_memory_space_constraint(a, pltpu.VMEM) for a in args[smem:])
    return pl.pallas_call(
        kernel,
        out_shape=out if last else jax.tree.map(lambda s: pltpu.VMEM(s.shape, s.dtype), out),
        in_specs=[SMEM] * smem + [VMEM] * (len(args) - smem),
        out_specs=jax.tree.map(lambda _: VMEM, out),
        scratch_shapes=scratch,
        compiler_params=pltpu.CompilerParams(vmem_limit_bytes=LIMIT),
        cost_estimate=pl.CostEstimate(flops=flops, bytes_accessed=1 << 22, transcendentals=0),
    )(*args)


def shape(dims, kind=f32):
    return jax.ShapeDtypeStruct(dims, kind)


def split_kernel(pos, h, v0, v1, mine, other, inv, top):
    core = pos[0]
    peak = jnp.maximum(jnp.max(jnp.abs(v0[...].astype(f32))), jnp.max(jnp.abs(v1[...].astype(f32))))
    top[...] = jnp.full((8, 128), peak, f32)

    def rows(i, _):
        at = pl.ds(pl.multiple_of(i * 32, 32), 32)
        total = jnp.zeros((32, 128), f32)
        for j in range(16):
            even = h[at, 256 * j : 256 * j + 128]
            odd = h[at, 256 * j + 128 : 256 * j + 256]
            wide_even, wide_odd = even.astype(f32), odd.astype(f32)
            total += wide_even * wide_even + wide_odd * wide_odd
            mine[at, 128 * j : 128 * j + 128] = jnp.where(core == 0, even, odd)
            other[at, 128 * j : 128 * j + 128] = jnp.where(core == 0, odd, even)
        mean = jnp.sum(total, axis=1, keepdims=True) * (1.0 / 4096)
        inv[at, :] = jnp.broadcast_to(lax.rsqrt(mean + epsilon), (32, 128))
        return 0

    lax.fori_loop(0, 8, rows, 0)


def over(rows):
    a, b, c, d = rows
    return jnp.maximum(jnp.maximum(a, b), jnp.maximum(c, d))


def own_kernel(gain, own, v, ring, far):
    ring[0:128, :] = own[...]
    far[0:256, :] = v[...]
    far[256:384, :] = own[...]
    g = gain[...]
    top = g.astype(bf16)
    rest = g - top.astype(f32)
    middle = rest.astype(bf16)
    low = (rest - middle.astype(f32)).astype(bf16)
    line = jnp.concatenate([top, middle, low, low], axis=1)
    ring[128:144, :] = jnp.broadcast_to(line, (16, 512))


def second_kernel(pos, gain, m1, p1, m2, t0, t1, t2, t3, out):
    low = pos[3]
    out[pl.ds(low, 1), :] = gain[...]
    for dz, r in ((3, m1), (1, p1), (2, m2)):
        line = r[128:144, :].astype(f32)
        out[pl.ds((low + dz) & 3, 1), :] = (line[0:1, 0:128] + line[0:1, 128:256]) + line[0:1, 256:384]
    out[4:5, :] = over([t[0:1, :] for t in (t0, t1, t2, t3)])


def gain_kernel(pos, r0, r1, r2, r3, out, power):
    y = pos[1]
    refs = (r0, r1, r2, r3)
    for b, r in enumerate(refs):
        for low in range(4):
            out[:, pl.ds(pl.multiple_of((low * 4 + (y ^ b)) * 128, 128), 128)] = r[low : low + 1, :]
    here = jnp.ceil(jnp.log2(jnp.maximum(r0[4:5, :], 1e-30)))
    wide = jnp.ceil(jnp.log2(jnp.maximum(over([r[4:5, :] for r in refs]), 1e-30))) + 2.0
    power[0:1, :] = jnp.exp2(-here)
    power[1:2, :] = jnp.exp2(here - wide)
    power[2:3, :] = jnp.exp2(wide) * (1.0 / 128)
    power[3:8, :] = jnp.zeros((5, 128), f32)


def tile(a, n):
    return jnp.concatenate([a] * n, axis=1)


def weight_kernel(pos, h0, h1, i0, i1, gain, power, v0, v1, out, vg):
    x, y, low = pos[4], pos[1], pos[3]
    vg[0:256, :] = v0[...]
    vg[256:512, :] = v1[...]
    scale = power[0:1, 0:1]
    for n in range(8):
        cols = slice(256 * n, 256 * n + 256)
        top_half = h0[:, cols].astype(f32) * tile(i0[...], 2) * gain[:, cols]
        low_half = h1[:, cols].astype(f32) * tile(i1[...], 2) * gain[:, cols]
        normed = jnp.concatenate([top_half.astype(bf16), low_half.astype(bf16)], axis=0)
        part = lax.dot_general(normed, vg[...], (((0,), (0,)), ((), ())), preferred_element_type=f32)
        part = part * scale
        for b in range(2):
            block = 2 * n + b
            row = pl.multiple_of(((((block % 4) ^ y) * 4) + ((block // 4) ^ low)) * 32, 32)
            for q in range(4):
                out[q ^ x, pl.ds(row, 32), :] = part[128 * b + 32 * q : 128 * b + 32 * q + 32, :]


def join_kernel(*refs):
    for at, (r, row) in enumerate(zip(refs[:-1], JOINED[len(refs)], strict=True)):
        refs[-1][128 * at : 128 * at + 128, :] = r[row : row + 128, :]


JOINED = {6: (0, 0, 0, 0, 0), 4: (0, 0, 256)}


def grad_kernel(pos, *refs):
    y, z, low = pos[1], pos[2], pos[3]
    (near, b1, b2, b3, far, c1, c2, c3, v0, v1, q4, u1, h0, h1, i0, i1, gain) = refs[:17]
    scaled, center, gain_sum, wide, vg = refs[17:]

    def place(value, dy, dz):
        there = lax.rem(z + dz + 8, 8)
        row = pl.multiple_of((lax.rem(there, 4) * 4 + (y ^ dy)) * 128, 128)
        wide[there // 4, pl.ds(row, 128), :] = value

    for dy, (n, f) in enumerate(((near, far), (b1, c1), (b2, c2), (b3, c3))):
        for i, dz in enumerate((0, -1, 1, -2, 2)):
            place(n[128 * i : 128 * i + 128, :], dy, dz)
        for i, dz in enumerate((-3, 3, 4)):
            place(f[128 * i : 128 * i + 128, :], dy, dz)
    high = z // 4
    for at, top, bottom in ((high, v0, v1), (1 - high, q4, u1)):
        vg[at, 0:256, :] = top[0:256, :]
        vg[at, 256:512, :] = bottom[0:256, :]

    total = [jnp.zeros((256, 128), f32), jnp.zeros((256, 128), f32)]
    for n in range(8):
        cols = slice(256 * n, 256 * n + 256)
        gain_part = jnp.zeros((1, 256), f32)
        for t, (h, i) in enumerate(((h0, i0), (h1, i1))):
            rows = slice(256 * t, 256 * t + 256)
            grad = lax.dot_general(vg[0, rows, :], wide[0, cols, :], (((1,), (1,)), ((), ())), preferred_element_type=f32)
            grad += lax.dot_general(vg[1, rows, :], wide[1, cols, :], (((1,), (1,)), ((), ())), preferred_element_type=f32)
            normal = h[:, cols].astype(f32) * tile(i[...], 2)
            gain_part += jnp.sum(grad * normal, axis=0, keepdims=True)
            by_gain = grad * gain[:, cols]
            scaled[rows, cols] = by_gain
            product = by_gain * normal
            total[t] += product[:, :128] + product[:, 128:]
        for b in range(2):
            block = 2 * n + b
            row = ((block % 4) ^ y) * 4 + ((block // 4) ^ low)
            gain_sum[pl.ds(row, 1), :] = gain_part[:, 128 * b : 128 * b + 128]
    for t in range(2):
        center[256 * t : 256 * t + 256, :] = jnp.broadcast_to(jnp.sum(total[t], axis=1, keepdims=True), (256, 128))


def input_kernel(scaled, c_here, c_there, h0, h1, i0, i1, mine, other):
    for t, (h, i, out) in enumerate(((h0, i0, mine), (h1, i1, other))):
        rows, across = slice(256 * t, 256 * t + 256), slice(256 - 256 * t, 512 - 256 * t)
        center = (c_here[rows, :] + c_there[across, :]) * (1.0 / 4096)
        inv = i[...]
        for j in range(16):
            cols = slice(128 * j, 128 * j + 128)
            normal = h[:, cols].astype(f32) * inv
            out[:, cols] = (inv * (scaled[rows, cols] - normal * center)).astype(bf16)


def merge_kernel(pos, mine, other, out):
    core = pos[0]
    for j in range(16):
        cols = slice(128 * j, 128 * j + 128)
        a, b = mine[:, cols], other[:, cols]
        out[:, 256 * j : 256 * j + 128] = jnp.where(core == 0, a, b)
        out[:, 256 * j + 128 : 256 * j + 256] = jnp.where(core == 0, b, a)


def tree(a, b, c, d):
    return (a + b) + (c + d)


def low_kernel(total, g0, g1, g2, g3, *outs):
    for k, out in enumerate(outs):
        out[0:32, :] = total[32 * k : 32 * k + 32, :]
        out[32:40, :] = jnp.zeros((8, 512), f32)
        out[32:33, 0:128] = tree(*(g[4 * j + k : 4 * j + k + 1, :] for j, g in enumerate((g0, g1, g2, g3))))


def sum_kernel(a, b, c, d, out):
    out[...] = tree(a[...], b[...], c[...], d[...])


def place_kernel(pos, r0, r1, r2, r3, out, gain):
    refs = (r0, r1, r2, r3)
    for k, r in enumerate(refs):
        row = pl.multiple_of((pos[4] ^ k) * 32, 32)
        out[pl.ds(row, 32), :] = r[0:32, :]
    gain[...] = tree(*(r[32:33, 0:128] for r in refs)) * (1.0 / 128)


def local(hidden, norm_gain, value_weight, value_grad):
    x, fsdp, high = lax.axis_index("rep"), lax.axis_index("fsdp"), lax.axis_index("tp")
    core, y, low = fsdp % 2, (fsdp // 2) % 4, fsdp // 8
    pos = jnp.stack([core, y, high * 4 + low, low, x]).astype(jnp.int32)
    message = shape((8, 128))
    half = shape((256, 2048), bf16)

    own, v0, gain_row = value_weight, value_grad, norm_gain.reshape(1, 128)
    v1 = send(v0, core=1)
    ring, ring4 = call(own_kernel, (shape((144, 512), bf16), shape((384, 512), bf16)), gain_row, own, v0)
    m1, p1 = send(ring, z=1), send(ring, z=-1)
    m2, p2 = send(ring, z=2), send(ring, z=-2)
    q4 = send(ring4, z=4)
    m3, p3 = send(m2, z=1), send(p2, z=-1)

    h0, give, i0, top = call(split_kernel, (half, half, shape((256, 128)), message), pos, hidden, v0, v1, smem=1)
    h1, i1 = send(give, core=1), send(i0, core=1)
    second = call(second_kernel, message, pos, gain_row, m1, p1, m2, top, *three([top] * 3, "x"), smem=1)
    gain, power = call(gain_kernel, (shape((1, 2048)), message), pos, second, *three([second] * 3, "y"), smem=1)

    near = call(join_kernel, shape((640, 512), bf16), own, m1, p1, m2, p2)
    b1, b3 = send(near, y=1), send(near, y=3)
    b2 = send(b1, y=3)
    far = call(join_kernel, shape((384, 512), bf16), m3, p3, q4)
    c1, c3 = send(far, y=1), send(far, y=3)
    c2 = send(c3, y=1)
    u1 = send(q4, core=1)

    part = call(
        weight_kernel,
        shape((4, 512, 512)),
        pos, h0, h1, i0, i1, gain, power, v0, v1,
        smem=1,
        scratch=[pltpu.VMEM((512, 512), bf16)],
        flops=2 * 512 * 512 * 2048,
    )
    got = three([part[k].astype(f16) for k in (1, 2, 3)], "x")
    total = tree(part[0], *(g.astype(f32) for g in got)) * power[1:2, 0:1]
    got = three([total[128 * k : 128 * k + 128].astype(f16) for k in (1, 2, 3)], "y")
    total = tree(total[:128], *(g.astype(f32) for g in got)) * power[2:3, 0:1]
    scaled, center, gain_part = call(
        grad_kernel,
        (shape((512, 2048)), shape((512, 128)), shape((16, 128))),
        pos, near, b1, b2, b3, far, c1, c2, c3, v0, v1, q4, u1, h0, h1, i0, i1, gain,
        smem=1,
        scratch=[pltpu.VMEM((2, 2048, 512), bf16), pltpu.VMEM((2, 512, 512), bf16)],
        flops=2 * 512 * 1024 * 2048,
    )
    across = send(center, core=1)
    mine, other = call(input_kernel, (half, half), scaled, center, across, h0, h1, i0, i1)
    input_grad = call(merge_kernel, shape((256, 4096), bf16), pos, mine, send(other, core=1), smem=1, last=True)

    row = shape((40, 512))
    lows = call(low_kernel, (row,) * 4, total, gain_part, *three([gain_part] * 3, "y"))
    final = call(sum_kernel, row, lows[0], *three(lows[1:], "low"))
    weight_grad, gain_grad = call(
        place_kernel,
        (shape((128, 512)), shape((1, 128))),
        pos, final, *three([final] * 3, "x"),
        smem=1,
        last=True,
    )
    return input_grad, weight_grad, gain_grad.reshape(128)


def solution(mesh):
    return jax.shard_map(
        local,
        mesh=mesh,
        in_specs=(P(("rep", "fsdp"), None), P("fsdp"), P("fsdp", "tp"), P(("rep", "fsdp"), "tp")),
        out_specs=(P(("rep", "fsdp"), None), P("fsdp", "tp"), P("fsdp")),
        check_vma=False,
    )
```

```python
import jax
import jax.numpy as jnp
from jax import lax
from jax.experimental import pallas as pl
from jax.experimental.pallas import tpu as pltpu
from jax.sharding import PartitionSpec as P

epsilon = 1e-05
AXES = ("rep", "fsdp", "tp")
LIMIT = 16 << 20
VMEM = pl.BlockSpec(memory_space=pltpu.VMEM)
SMEM = pl.BlockSpec(memory_space=pltpu.SMEM)
f32, bf16, f16 = jnp.float32, jnp.bfloat16, jnp.float16


def permutation(move):
    pairs = []
    for x in range(4):
        for low in range(4):
            for y in range(4):
                for core in range(2):
                    for high in range(2):
                        tx, ty, tz, tc = move(x, y, high * 4 + low, core)
                        source = (x * 32 + low * 8 + y * 2 + core) * 2 + high
                        target = (tx * 32 + (tz % 4) * 8 + ty * 2 + tc) * 2 + tz // 4
                        pairs.append((source, target))
    return pairs


def send(value, x=0, y=0, z=0, low=0, core=0):
    def move(px, py, pz, pc):
        tz = (pz + z) % 8
        return px ^ x, py ^ y, (tz // 4) * 4 + ((tz % 4) ^ low), pc ^ core

    return lax.ppermute(value, AXES, permutation(move))


def three(values, axis):
    return [send(values[k - 1], **{axis: k}) for k in (1, 2, 3)]


def call(kernel, out, *args, smem=0, scratch=(), flops=0, last=False):
    args = args[:smem] + tuple(pltpu.with_memory_space_constraint(a, pltpu.VMEM) for a in args[smem:])
    return pl.pallas_call(
        kernel,
        out_shape=out if last else jax.tree.map(lambda s: pltpu.VMEM(s.shape, s.dtype), out),
        in_specs=[SMEM] * smem + [VMEM] * (len(args) - smem),
        out_specs=jax.tree.map(lambda _: VMEM, out),
        scratch_shapes=scratch,
        compiler_params=pltpu.CompilerParams(vmem_limit_bytes=LIMIT),
        cost_estimate=pl.CostEstimate(flops=flops, bytes_accessed=1 << 22, transcendentals=0),
    )(*args)


def shape(dims, kind=f32):
    return jax.ShapeDtypeStruct(dims, kind)


def split_kernel(pos, h, v0, v1, mine, other, inv, top):
    core = pos[0]
    peak = jnp.maximum(jnp.max(jnp.abs(v0[...].astype(f32))), jnp.max(jnp.abs(v1[...].astype(f32))))
    top[...] = jnp.full((8, 128), peak, f32)

    def rows(i, _):
        at = pl.ds(pl.multiple_of(i * 32, 32), 32)
        total = jnp.zeros((32, 128), f32)
        for j in range(16):
            even = h[at, 256 * j : 256 * j + 128]
            odd = h[at, 256 * j + 128 : 256 * j + 256]
            wide_even, wide_odd = even.astype(f32), odd.astype(f32)
            total += wide_even * wide_even + wide_odd * wide_odd
            mine[at, 128 * j : 128 * j + 128] = jnp.where(core == 0, even, odd)
            other[at, 128 * j : 128 * j + 128] = jnp.where(core == 0, odd, even)
        mean = jnp.sum(total, axis=1, keepdims=True) * (1.0 / 4096)
        inv[at, :] = jnp.broadcast_to(lax.rsqrt(mean + epsilon), (32, 128))
        return 0

    lax.fori_loop(0, 8, rows, 0)


def over(rows):
    a, b, c, d = rows
    return jnp.maximum(jnp.maximum(a, b), jnp.maximum(c, d))


def own_kernel(gain, own, ring):
    ring[0:128, :] = own[...]
    g = gain[...]
    top = g.astype(bf16)
    rest = g - top.astype(f32)
    middle = rest.astype(bf16)
    low = (rest - middle.astype(f32)).astype(bf16)
    line = jnp.concatenate([top, middle, low, low], axis=1)
    ring[128:144, :] = jnp.broadcast_to(line, (16, 512))


def second_kernel(pos, gain, m1, p1, m2, t0, t1, t2, t3, out):
    low = pos[3]
    out[pl.ds(low, 1), :] = gain[...]
    for dz, r in ((3, m1), (1, p1), (2, m2)):
        line = r[128:144, :].astype(f32)
        out[pl.ds((low + dz) & 3, 1), :] = (line[0:1, 0:128] + line[0:1, 128:256]) + line[0:1, 256:384]
    out[4:5, :] = over([t[0:1, :] for t in (t0, t1, t2, t3)])


def gain_kernel(pos, r0, r1, r2, r3, out, power):
    y = pos[1]
    refs = (r0, r1, r2, r3)
    for b, r in enumerate(refs):
        for low in range(4):
            out[:, pl.ds(pl.multiple_of((low * 4 + (y ^ b)) * 128, 128), 128)] = r[low : low + 1, :]
    here = jnp.ceil(jnp.log2(jnp.maximum(r0[4:5, :], 1e-30)))
    wide = jnp.ceil(jnp.log2(jnp.maximum(over([r[4:5, :] for r in refs]), 1e-30))) + 2.0
    power[0:1, :] = jnp.exp2(-here)
    power[1:2, :] = jnp.exp2(here - wide)
    power[2:3, :] = jnp.exp2(wide) * (1.0 / 128)
    power[3:8, :] = jnp.zeros((5, 128), f32)


def tile(a, n):
    return jnp.concatenate([a] * n, axis=1)


def weight_kernel(pos, h0, h1, i0, i1, gain, power, v0, v1, out, vg):
    x, y, low = pos[4], pos[1], pos[3]
    vg[0:256, :] = v0[...]
    vg[256:512, :] = v1[...]
    scale = power[0:1, 0:1]
    for n in range(8):
        cols = slice(256 * n, 256 * n + 256)
        top_half = h0[:, cols].astype(f32) * tile(i0[...], 2) * gain[:, cols]
        low_half = h1[:, cols].astype(f32) * tile(i1[...], 2) * gain[:, cols]
        normed = jnp.concatenate([top_half.astype(bf16), low_half.astype(bf16)], axis=0)
        part = lax.dot_general(normed, vg[...], (((0,), (0,)), ((), ())), preferred_element_type=f32)
        part = part * scale
        for b in range(2):
            block = 2 * n + b
            row = pl.multiple_of(((((block % 4) ^ y) * 4) + ((block // 4) ^ low)) * 32, 32)
            for q in range(4):
                out[q ^ x, pl.ds(row, 32), :] = part[128 * b + 32 * q : 128 * b + 32 * q + 32, :]


def join_kernel(*refs):
    for at, r in enumerate(refs[:-1]):
        refs[-1][128 * at : 128 * at + 128, :] = r[0:128, :]


def grad_kernel(pos, *refs):
    y, z, low = pos[1], pos[2], pos[3]
    (own, a1, a2, a3, near, b1, b2, b3, far, c1, c2, c3, v0, v1, u0, u1, h0, h1, i0, i1, gain) = refs[:21]
    scaled, center, gain_sum, wide, vg = refs[21:]

    def place(value, dy, dz):
        there = lax.rem(z + dz + 8, 8)
        row = pl.multiple_of((lax.rem(there, 4) * 4 + (y ^ dy)) * 128, 128)
        wide[there // 4, pl.ds(row, 128), :] = value

    for dy, (o, n, f) in enumerate(((own, near, far), (a1, b1, c1), (a2, b2, c2), (a3, b3, c3))):
        place(o[...], dy, 0)
        for i, dz in enumerate((-1, 1, -2, 2)):
            place(n[128 * i : 128 * i + 128, :], dy, dz)
        for i, dz in enumerate((-3, 3, 4)):
            place(f[128 * i : 128 * i + 128, :], dy, dz)
    high = z // 4
    for at, top, bottom in ((high, v0, v1), (1 - high, u0, u1)):
        vg[at, 0:256, :] = top[...]
        vg[at, 256:512, :] = bottom[...]

    total = [jnp.zeros((256, 128), f32), jnp.zeros((256, 128), f32)]
    for n in range(8):
        cols = slice(256 * n, 256 * n + 256)
        gain_part = jnp.zeros((1, 256), f32)
        for t, (h, i) in enumerate(((h0, i0), (h1, i1))):
            rows = slice(256 * t, 256 * t + 256)
            grad = lax.dot_general(vg[0, rows, :], wide[0, cols, :], (((1,), (1,)), ((), ())), preferred_element_type=f32)
            grad += lax.dot_general(vg[1, rows, :], wide[1, cols, :], (((1,), (1,)), ((), ())), preferred_element_type=f32)
            normal = h[:, cols].astype(f32) * tile(i[...], 2)
            gain_part += jnp.sum(grad * normal, axis=0, keepdims=True)
            by_gain = grad * gain[:, cols]
            scaled[rows, cols] = by_gain
            product = by_gain * normal
            total[t] += product[:, :128] + product[:, 128:]
        for b in range(2):
            block = 2 * n + b
            row = ((block % 4) ^ y) * 4 + ((block // 4) ^ low)
            gain_sum[pl.ds(row, 1), :] = gain_part[:, 128 * b : 128 * b + 128]
    for t in range(2):
        center[256 * t : 256 * t + 256, :] = jnp.broadcast_to(jnp.sum(total[t], axis=1, keepdims=True), (256, 128))


def input_kernel(scaled, c_here, c_there, h0, h1, i0, i1, mine, other):
    for t, (h, i, out) in enumerate(((h0, i0, mine), (h1, i1, other))):
        rows, across = slice(256 * t, 256 * t + 256), slice(256 - 256 * t, 512 - 256 * t)
        center = (c_here[rows, :] + c_there[across, :]) * (1.0 / 4096)
        inv = i[...]
        for j in range(16):
            cols = slice(128 * j, 128 * j + 128)
            normal = h[:, cols].astype(f32) * inv
            out[:, cols] = (inv * (scaled[rows, cols] - normal * center)).astype(bf16)


def merge_kernel(pos, mine, other, out):
    core = pos[0]
    for j in range(16):
        cols = slice(128 * j, 128 * j + 128)
        a, b = mine[:, cols], other[:, cols]
        out[:, 256 * j : 256 * j + 128] = jnp.where(core == 0, a, b)
        out[:, 256 * j + 128 : 256 * j + 256] = jnp.where(core == 0, b, a)


def tree(a, b, c, d):
    return (a + b) + (c + d)


def low_kernel(total, g0, g1, g2, g3, *outs):
    for k, out in enumerate(outs):
        out[0:32, :] = total[32 * k : 32 * k + 32, :]
        out[32:40, :] = jnp.zeros((8, 512), f32)
        out[32:33, 0:128] = tree(*(g[4 * j + k : 4 * j + k + 1, :] for j, g in enumerate((g0, g1, g2, g3))))


def sum_kernel(a, b, c, d, out):
    out[...] = tree(a[...], b[...], c[...], d[...])


def place_kernel(pos, r0, r1, r2, r3, out, gain):
    refs = (r0, r1, r2, r3)
    for k, r in enumerate(refs):
        row = pl.multiple_of((pos[4] ^ k) * 32, 32)
        out[pl.ds(row, 32), :] = r[0:32, :]
    gain[...] = tree(*(r[32:33, 0:128] for r in refs)) * (1.0 / 128)


def local(hidden, norm_gain, value_weight, value_grad):
    x, fsdp, high = lax.axis_index("rep"), lax.axis_index("fsdp"), lax.axis_index("tp")
    core, y, low = fsdp % 2, (fsdp // 2) % 4, fsdp // 8
    pos = jnp.stack([core, y, high * 4 + low, low, x]).astype(jnp.int32)
    message = shape((8, 128))
    half = shape((256, 2048), bf16)

    own, v0, gain_row = value_weight, value_grad, norm_gain.reshape(1, 128)
    v1 = send(v0, core=1)
    a1, a3 = send(own, y=1), send(own, y=3)
    a2 = send(a1, y=3)
    ring = call(own_kernel, shape((144, 512), bf16), gain_row, own)
    m1, p1 = send(ring, z=1), send(ring, z=-1)
    m2, p2 = send(m1, z=1), send(p1, z=-1)
    m3, p3 = send(m2, z=1), send(p2, z=-1)
    q4 = send(m3, z=1)
    u0 = send(v0, z=4)
    u1 = send(u0, core=1)

    h0, give, i0, top = call(split_kernel, (half, half, shape((256, 128)), message), pos, hidden, v0, v1, smem=1)
    h1, i1 = send(give, core=1), send(i0, core=1)
    second = call(second_kernel, message, pos, gain_row, m1, p1, m2, top, *three([top] * 3, "x"), smem=1)
    gain, power = call(gain_kernel, (shape((1, 2048)), message), pos, second, *three([second] * 3, "y"), smem=1)

    near = call(join_kernel, shape((512, 512), bf16), m1, p1, m2, p2)
    b1, b3 = send(near, y=1), send(near, y=3)
    b2 = send(b1, y=3)
    far = call(join_kernel, shape((384, 512), bf16), m3, p3, q4)
    c1, c3 = send(far, y=1), send(far, y=3)
    c2 = send(c3, y=1)

    part = call(
        weight_kernel,
        shape((4, 512, 512)),
        pos, h0, h1, i0, i1, gain, power, v0, v1,
        smem=1,
        scratch=[pltpu.VMEM((512, 512), bf16)],
        flops=2 * 512 * 512 * 2048,
    )
    got = three([part[k].astype(f16) for k in (1, 2, 3)], "x")
    total = tree(part[0], *(g.astype(f32) for g in got)) * power[1:2, 0:1]
    got = three([total[128 * k : 128 * k + 128].astype(f16) for k in (1, 2, 3)], "y")
    total = tree(total[:128], *(g.astype(f32) for g in got)) * power[2:3, 0:1]
    scaled, center, gain_part = call(
        grad_kernel,
        (shape((512, 2048)), shape((512, 128)), shape((16, 128))),
        pos, own, a1, a2, a3, near, b1, b2, b3, far, c1, c2, c3, v0, v1, u0, u1, h0, h1, i0, i1, gain,
        smem=1,
        scratch=[pltpu.VMEM((2, 2048, 512), bf16), pltpu.VMEM((2, 512, 512), bf16)],
        flops=2 * 512 * 1024 * 2048,
    )
    across = send(center, core=1)
    mine, other = call(input_kernel, (half, half), scaled, center, across, h0, h1, i0, i1)
    input_grad = call(merge_kernel, shape((256, 4096), bf16), pos, mine, send(other, core=1), smem=1, last=True)

    row = shape((40, 512))
    lows = call(low_kernel, (row,) * 4, total, gain_part, *three([gain_part] * 3, "y"))
    final = call(sum_kernel, row, lows[0], *three(lows[1:], "low"))
    weight_grad, gain_grad = call(
        place_kernel,
        (shape((128, 512)), shape((1, 128))),
        pos, final, *three([final] * 3, "x"),
        smem=1,
        last=True,
    )
    return input_grad, weight_grad, gain_grad.reshape(128)


def solution(mesh):
    return jax.shard_map(
        local,
        mesh=mesh,
        in_specs=(P(("rep", "fsdp"), None), P("fsdp"), P("fsdp", "tp"), P(("rep", "fsdp"), "tp")),
        out_specs=(P(("rep", "fsdp"), None), P("fsdp", "tp"), P("fsdp")),
        check_vma=False,
    )
```

```python
import jax
import jax.numpy as jnp
from jax import lax
from jax.experimental import pallas as pl
from jax.experimental.pallas import tpu as pltpu
from jax.sharding import PartitionSpec as P

epsilon = 1e-05
AXES = ("rep", "fsdp", "tp")
LIMIT = 16 << 20
VMEM = pl.BlockSpec(memory_space=pltpu.VMEM)
SMEM = pl.BlockSpec(memory_space=pltpu.SMEM)
f32, bf16, f16 = jnp.float32, jnp.bfloat16, jnp.float16


def permutation(move):
    pairs = []
    for x in range(4):
        for low in range(4):
            for y in range(4):
                for core in range(2):
                    for high in range(2):
                        tx, ty, tz, tc = move(x, y, high * 4 + low, core)
                        source = (x * 32 + low * 8 + y * 2 + core) * 2 + high
                        target = (tx * 32 + (tz % 4) * 8 + ty * 2 + tc) * 2 + tz // 4
                        pairs.append((source, target))
    return pairs


def send(value, x=0, y=0, z=0, low=0, core=0):
    def move(px, py, pz, pc):
        tz = (pz + z) % 8
        return px ^ x, py ^ y, (tz // 4) * 4 + ((tz % 4) ^ low), pc ^ core

    return lax.ppermute(value, AXES, permutation(move))


def three(values, axis):
    return [send(values[k - 1], **{axis: k}) for k in (1, 2, 3)]


def call(kernel, out, *args, smem=0, scratch=(), flops=0, last=False):
    args = args[:smem] + tuple(pltpu.with_memory_space_constraint(a, pltpu.VMEM) for a in args[smem:])
    return pl.pallas_call(
        kernel,
        out_shape=out if last else jax.tree.map(lambda s: pltpu.VMEM(s.shape, s.dtype), out),
        in_specs=[SMEM] * smem + [VMEM] * (len(args) - smem),
        out_specs=jax.tree.map(lambda _: VMEM, out),
        scratch_shapes=scratch,
        compiler_params=pltpu.CompilerParams(vmem_limit_bytes=LIMIT),
        cost_estimate=pl.CostEstimate(flops=flops, bytes_accessed=1 << 22, transcendentals=0),
    )(*args)


def shape(dims, kind=f32):
    return jax.ShapeDtypeStruct(dims, kind)


def split_kernel(pos, h, v0, v1, mine, other, inv, top):
    core = pos[0]
    peak = jnp.maximum(jnp.max(jnp.abs(v0[...].astype(f32))), jnp.max(jnp.abs(v1[...].astype(f32))))
    top[...] = jnp.full((8, 128), peak, f32)

    def rows(i, _):
        at = pl.ds(pl.multiple_of(i * 32, 32), 32)
        total = jnp.zeros((32, 128), f32)
        for j in range(16):
            even = h[at, 256 * j : 256 * j + 128]
            odd = h[at, 256 * j + 128 : 256 * j + 256]
            wide_even, wide_odd = even.astype(f32), odd.astype(f32)
            total += wide_even * wide_even + wide_odd * wide_odd
            mine[at, 128 * j : 128 * j + 128] = jnp.where(core == 0, even, odd)
            other[at, 128 * j : 128 * j + 128] = jnp.where(core == 0, odd, even)
        mean = jnp.sum(total, axis=1, keepdims=True) * (1.0 / 4096)
        inv[at, :] = jnp.broadcast_to(lax.rsqrt(mean + epsilon), (32, 128))
        return 0

    lax.fori_loop(0, 8, rows, 0)


def over(rows):
    a, b, c, d = rows
    return jnp.maximum(jnp.maximum(a, b), jnp.maximum(c, d))


def own_kernel(gain, own, ring):
    ring[0:128, :] = own[...]
    g = gain[...]
    top = g.astype(bf16)
    rest = g - top.astype(f32)
    middle = rest.astype(bf16)
    low = (rest - middle.astype(f32)).astype(bf16)
    line = jnp.concatenate([top, middle, low, low], axis=1)
    ring[128:144, :] = jnp.broadcast_to(line, (16, 512))


def second_kernel(pos, gain, m1, p1, m2, out):
    low = pos[3]
    out[pl.ds(low, 1), :] = gain[...]
    for dz, r in ((3, m1), (1, p1), (2, m2)):
        line = r[128:144, :].astype(f32)
        out[pl.ds((low + dz) & 3, 1), :] = (line[0:1, 0:128] + line[0:1, 128:256]) + line[0:1, 256:384]


def gain_kernel(pos, r0, r1, r2, r3, out):
    y = pos[1]
    for b, r in enumerate((r0, r1, r2, r3)):
        for low in range(4):
            out[:, pl.ds(pl.multiple_of((low * 4 + (y ^ b)) * 128, 128), 128)] = r[low : low + 1, :]


def exponent(top):
    return jnp.ceil(jnp.log2(jnp.maximum(top, 1e-30)))


def top_kernel(a, b, c, d, out):
    out[...] = over([r[...] for r in (a, b, c, d)])


def scale_kernel(t0, t1, t2, t3, s0, s1, s2, s3, power):
    wide = exponent(over([r[0:1, :] for r in (s0, s1, s2, s3)])) + 2.0
    for k, r in enumerate((t0, t1, t2, t3)):
        power[k : k + 1, :] = jnp.exp2(exponent(r[0:1, :]) - wide)
    power[4:5, :] = jnp.exp2(wide) * (1.0 / 128)
    power[5:8, :] = jnp.zeros((3, 128), f32)


def tile(a, n):
    return jnp.concatenate([a] * n, axis=1)


def weight_kernel(pos, h0, h1, i0, i1, gain, top, v0, v1, out, vg):
    x, y, low = pos[4], pos[1], pos[3]
    vg[0:256, :] = v0[...]
    vg[256:512, :] = v1[...]
    scale = jnp.exp2(-exponent(top[0:1, :]))[0:1, 0:1]
    for n in range(8):
        cols = slice(256 * n, 256 * n + 256)
        top_half = h0[:, cols].astype(f32) * tile(i0[...], 2) * gain[:, cols]
        low_half = h1[:, cols].astype(f32) * tile(i1[...], 2) * gain[:, cols]
        normed = jnp.concatenate([top_half.astype(bf16), low_half.astype(bf16)], axis=0)
        part = lax.dot_general(normed, vg[...], (((0,), (0,)), ((), ())), preferred_element_type=f32)
        part = part * scale
        for b in range(2):
            block = 2 * n + b
            row = pl.multiple_of(((((block % 4) ^ y) * 4) + ((block // 4) ^ low)) * 32, 32)
            for q in range(4):
                out[q ^ x, pl.ds(row, 32), :] = part[128 * b + 32 * q : 128 * b + 32 * q + 32, :]


def join_kernel(*refs):
    for at, r in enumerate(refs[:-1]):
        refs[-1][128 * at : 128 * at + 128, :] = r[0:128, :]


def grad_kernel(pos, *refs):
    y, z, low = pos[1], pos[2], pos[3]
    (own, a1, a2, a3, near, b1, b2, b3, far, c1, c2, c3, v0, v1, u0, u1, h0, h1, i0, i1, gain) = refs[:21]
    scaled, center, gain_sum, wide, vg = refs[21:]

    def place(value, dy, dz):
        there = lax.rem(z + dz + 8, 8)
        row = pl.multiple_of((lax.rem(there, 4) * 4 + (y ^ dy)) * 128, 128)
        wide[there // 4, pl.ds(row, 128), :] = value

    for dy, (o, n, f) in enumerate(((own, near, far), (a1, b1, c1), (a2, b2, c2), (a3, b3, c3))):
        place(o[...], dy, 0)
        for i, dz in enumerate((-1, 1, -2, 2)):
            place(n[128 * i : 128 * i + 128, :], dy, dz)
        for i, dz in enumerate((-3, 3, 4)):
            place(f[128 * i : 128 * i + 128, :], dy, dz)
    high = z // 4
    for at, top, bottom in ((high, v0, v1), (1 - high, u0, u1)):
        vg[at, 0:256, :] = top[...]
        vg[at, 256:512, :] = bottom[...]

    total = [jnp.zeros((256, 128), f32), jnp.zeros((256, 128), f32)]
    for n in range(8):
        cols = slice(256 * n, 256 * n + 256)
        gain_part = jnp.zeros((1, 256), f32)
        for t, (h, i) in enumerate(((h0, i0), (h1, i1))):
            rows = slice(256 * t, 256 * t + 256)
            grad = lax.dot_general(vg[0, rows, :], wide[0, cols, :], (((1,), (1,)), ((), ())), preferred_element_type=f32)
            grad += lax.dot_general(vg[1, rows, :], wide[1, cols, :], (((1,), (1,)), ((), ())), preferred_element_type=f32)
            normal = h[:, cols].astype(f32) * tile(i[...], 2)
            gain_part += jnp.sum(grad * normal, axis=0, keepdims=True)
            by_gain = grad * gain[:, cols]
            scaled[rows, cols] = by_gain
            product = by_gain * normal
            total[t] += product[:, :128] + product[:, 128:]
        for b in range(2):
            block = 2 * n + b
            row = ((block % 4) ^ y) * 4 + ((block // 4) ^ low)
            gain_sum[pl.ds(row, 1), :] = gain_part[:, 128 * b : 128 * b + 128]
    for t in range(2):
        center[256 * t : 256 * t + 256, :] = jnp.broadcast_to(jnp.sum(total[t], axis=1, keepdims=True), (256, 128))


def input_kernel(scaled, c_here, c_there, h0, h1, i0, i1, mine, other):
    for t, (h, i, out) in enumerate(((h0, i0, mine), (h1, i1, other))):
        rows, across = slice(256 * t, 256 * t + 256), slice(256 - 256 * t, 512 - 256 * t)
        center = (c_here[rows, :] + c_there[across, :]) * (1.0 / 4096)
        inv = i[...]
        for j in range(16):
            cols = slice(128 * j, 128 * j + 128)
            normal = h[:, cols].astype(f32) * inv
            out[:, cols] = (inv * (scaled[rows, cols] - normal * center)).astype(bf16)


def merge_kernel(pos, mine, other, out):
    core = pos[0]
    for j in range(16):
        cols = slice(128 * j, 128 * j + 128)
        a, b = mine[:, cols], other[:, cols]
        out[:, 256 * j : 256 * j + 128] = jnp.where(core == 0, a, b)
        out[:, 256 * j + 128 : 256 * j + 256] = jnp.where(core == 0, b, a)


def tree(a, b, c, d):
    return (a + b) + (c + d)


def low_kernel(total, g0, g1, g2, g3, *outs):
    for k, out in enumerate(outs):
        out[0:32, :] = total[32 * k : 32 * k + 32, :]
        out[32:40, :] = jnp.zeros((8, 512), f32)
        out[32:33, 0:128] = tree(*(g[4 * j + k : 4 * j + k + 1, :] for j, g in enumerate((g0, g1, g2, g3))))


def sum_kernel(a, b, c, d, out):
    out[...] = tree(a[...], b[...], c[...], d[...])


def place_kernel(pos, r0, r1, r2, r3, out, gain):
    refs = (r0, r1, r2, r3)
    for k, r in enumerate(refs):
        row = pl.multiple_of((pos[4] ^ k) * 32, 32)
        out[pl.ds(row, 32), :] = r[0:32, :]
    gain[...] = tree(*(r[32:33, 0:128] for r in refs)) * (1.0 / 128)


def local(hidden, norm_gain, value_weight, value_grad):
    x, fsdp, high = lax.axis_index("rep"), lax.axis_index("fsdp"), lax.axis_index("tp")
    core, y, low = fsdp % 2, (fsdp // 2) % 4, fsdp // 8
    pos = jnp.stack([core, y, high * 4 + low, low, x]).astype(jnp.int32)
    message = shape((8, 128))
    half = shape((256, 2048), bf16)

    own, v0, gain_row = value_weight, value_grad, norm_gain.reshape(1, 128)
    v1 = send(v0, core=1)
    a1, a3 = send(own, y=1), send(own, y=3)
    a2 = send(a1, y=3)
    ring = call(own_kernel, shape((144, 512), bf16), gain_row, own)
    m1, p1 = send(ring, z=1), send(ring, z=-1)
    m2, p2 = send(m1, z=1), send(p1, z=-1)
    m3, p3 = send(m2, z=1), send(p2, z=-1)
    q4 = send(m3, z=1)
    u0 = send(v0, z=4)
    u1 = send(u0, core=1)

    h0, give, i0, top = call(split_kernel, (half, half, shape((256, 128)), message), pos, hidden, v0, v1, smem=1)
    h1, i1 = send(give, core=1), send(i0, core=1)
    second = call(second_kernel, message, pos, gain_row, m1, p1, m2, smem=1)
    gain = call(gain_kernel, shape((1, 2048)), pos, second, *three([second] * 3, "y"), smem=1)

    near = call(join_kernel, shape((512, 512), bf16), m1, p1, m2, p2)
    b1, b3 = send(near, y=1), send(near, y=3)
    b2 = send(b1, y=3)
    far = call(join_kernel, shape((384, 512), bf16), m3, p3, q4)
    c1, c3 = send(far, y=1), send(far, y=3)
    c2 = send(c3, y=1)

    part = call(
        weight_kernel,
        shape((4, 512, 512)),
        pos, h0, h1, i0, i1, gain, top, v0, v1,
        smem=1,
        scratch=[pltpu.VMEM((512, 512), bf16)],
        flops=2 * 512 * 512 * 2048,
    )
    got = three([part[k].astype(f16) for k in (1, 2, 3)], "x")
    tops = [top, *three([top] * 3, "x")]
    peak = call(top_kernel, message, *tops)
    power = call(scale_kernel, message, *tops, peak, *three([peak] * 3, "y"))
    total = tree(*(g.astype(f32) * power[k : k + 1, 0:1] for k, g in enumerate([part[0], *got])))
    got = three([total[128 * k : 128 * k + 128].astype(f16) for k in (1, 2, 3)], "y")
    total = tree(total[:128], *(g.astype(f32) for g in got)) * power[4:5, 0:1]
    scaled, center, gain_part = call(
        grad_kernel,
        (shape((512, 2048)), shape((512, 128)), shape((16, 128))),
        pos, own, a1, a2, a3, near, b1, b2, b3, far, c1, c2, c3, v0, v1, u0, u1, h0, h1, i0, i1, gain,
        smem=1,
        scratch=[pltpu.VMEM((2, 2048, 512), bf16), pltpu.VMEM((2, 512, 512), bf16)],
        flops=2 * 512 * 1024 * 2048,
    )
    across = send(center, core=1)
    mine, other = call(input_kernel, (half, half), scaled, center, across, h0, h1, i0, i1)
    input_grad = call(merge_kernel, shape((256, 4096), bf16), pos, mine, send(other, core=1), smem=1, last=True)

    row = shape((40, 512))
    lows = call(low_kernel, (row,) * 4, total, gain_part, *three([gain_part] * 3, "y"))
    final = call(sum_kernel, row, lows[0], *three(lows[1:], "low"))
    weight_grad, gain_grad = call(
        place_kernel,
        (shape((128, 512)), shape((1, 128))),
        pos, final, *three([final] * 3, "x"),
        smem=1,
        last=True,
    )
    return input_grad, weight_grad, gain_grad.reshape(128)


def solution(mesh):
    return jax.shard_map(
        local,
        mesh=mesh,
        in_specs=(P(("rep", "fsdp"), None), P("fsdp"), P("fsdp", "tp"), P(("rep", "fsdp"), "tp")),
        out_specs=(P(("rep", "fsdp"), None), P("fsdp", "tp"), P("fsdp")),
        check_vma=False,
    )
```

```python
import jax
import jax.numpy as jnp
from jax import lax
from jax.experimental import pallas as pl
from jax.experimental.pallas import tpu as pltpu
from jax.sharding import PartitionSpec as P

epsilon = 1e-05
AXES = ("rep", "fsdp", "tp")
LIMIT = 16 << 20
VMEM = pl.BlockSpec(memory_space=pltpu.VMEM)
SMEM = pl.BlockSpec(memory_space=pltpu.SMEM)
f32, bf16, f16 = jnp.float32, jnp.bfloat16, jnp.float16


def permutation(move):
    pairs = []
    for x in range(4):
        for low in range(4):
            for y in range(4):
                for core in range(2):
                    for high in range(2):
                        tx, ty, tz, tc = move(x, y, high * 4 + low, core)
                        source = (x * 32 + low * 8 + y * 2 + core) * 2 + high
                        target = (tx * 32 + (tz % 4) * 8 + ty * 2 + tc) * 2 + tz // 4
                        pairs.append((source, target))
    return pairs


def send(value, x=0, y=0, z=0, low=0, core=0):
    def move(px, py, pz, pc):
        tz = (pz + z) % 8
        return px ^ x, py ^ y, (tz // 4) * 4 + ((tz % 4) ^ low), pc ^ core

    return lax.ppermute(value, AXES, permutation(move))


def three(values, axis):
    return [send(values[k - 1], **{axis: k}) for k in (1, 2, 3)]


def call(kernel, out, *args, smem=0, scratch=(), flops=0, last=False):
    args = args[:smem] + tuple(pltpu.with_memory_space_constraint(a, pltpu.VMEM) for a in args[smem:])
    return pl.pallas_call(
        kernel,
        out_shape=out if last else jax.tree.map(lambda s: pltpu.VMEM(s.shape, s.dtype), out),
        in_specs=[SMEM] * smem + [VMEM] * (len(args) - smem),
        out_specs=jax.tree.map(lambda _: VMEM, out),
        scratch_shapes=scratch,
        compiler_params=pltpu.CompilerParams(vmem_limit_bytes=LIMIT),
        cost_estimate=pl.CostEstimate(flops=flops, bytes_accessed=1 << 22, transcendentals=0),
    )(*args)


def shape(dims, kind=f32):
    return jax.ShapeDtypeStruct(dims, kind)


def split_kernel(pos, h, mine, other, inv):
    core = pos[0]

    def rows(i, _):
        at = pl.ds(pl.multiple_of(i * 32, 32), 32)
        total = jnp.zeros((32, 128), f32)
        for j in range(16):
            even = h[at, 256 * j : 256 * j + 128]
            odd = h[at, 256 * j + 128 : 256 * j + 256]
            wide_even, wide_odd = even.astype(f32), odd.astype(f32)
            total += wide_even * wide_even + wide_odd * wide_odd
            mine[at, 128 * j : 128 * j + 128] = jnp.where(core == 0, even, odd)
            other[at, 128 * j : 128 * j + 128] = jnp.where(core == 0, odd, even)
        mean = jnp.sum(total, axis=1, keepdims=True) * (1.0 / 4096)
        inv[at, :] = jnp.broadcast_to(lax.rsqrt(mean + epsilon), (32, 128))
        return 0

    lax.fori_loop(0, 8, rows, 0)


def over(rows):
    a, b, c, d = rows
    return jnp.maximum(jnp.maximum(a, b), jnp.maximum(c, d))


def own_kernel(gain, own, ring):
    ring[0:128, :] = own[...]
    g = gain[...]
    top = g.astype(bf16)
    rest = g - top.astype(f32)
    middle = rest.astype(bf16)
    low = (rest - middle.astype(f32)).astype(bf16)
    line = jnp.concatenate([top, middle, low, low], axis=1)
    ring[128:144, :] = jnp.broadcast_to(line, (16, 512))


def second_kernel(pos, gain, m1, p1, m2, v0, v1, out):
    low = pos[3]
    out[pl.ds(low, 1), :] = gain[...]
    for dz, r in ((3, m1), (1, p1), (2, m2)):
        line = r[128:144, :].astype(f32)
        out[pl.ds((low + dz) & 3, 1), :] = (line[0:1, 0:128] + line[0:1, 128:256]) + line[0:1, 256:384]
    peak = jnp.maximum(jnp.max(jnp.abs(v0[...].astype(f32))), jnp.max(jnp.abs(v1[...].astype(f32))))
    out[4:8, :] = jnp.full((4, 128), peak, f32)


def gain_kernel(pos, r0, r1, r2, r3, out, top):
    y = pos[1]
    refs = (r0, r1, r2, r3)
    for b, r in enumerate(refs):
        for low in range(4):
            out[:, pl.ds(pl.multiple_of((low * 4 + (y ^ b)) * 128, 128), 128)] = r[low : low + 1, :]
    top[0:4, :] = r0[4:8, :]
    top[4:8, :] = over([r[4:8, :] for r in refs])


def exponent(top):
    return jnp.ceil(jnp.log2(jnp.maximum(top, 1e-30)))


def scale_kernel(t0, t1, t2, t3, power):
    refs = (t0, t1, t2, t3)
    wide = exponent(over([r[4:5, :] for r in refs])) + 2.0
    for k, r in enumerate(refs):
        power[k : k + 1, :] = tile(jnp.exp2(exponent(r[0:1, :]) - wide), 4)
    power[4:8, :] = jnp.broadcast_to(tile(jnp.exp2(wide) * (1.0 / 128), 4), (4, 512))


def tile(a, n):
    return jnp.concatenate([a] * n, axis=1)


def weight_kernel(pos, h0, h1, i0, i1, gain, top, v0, v1, out, vg):
    x, y, low = pos[4], pos[1], pos[3]
    vg[0:256, :] = v0[...]
    vg[256:512, :] = v1[...]
    scale = jnp.exp2(-exponent(top[0:1, :]))[0:1, 0:1]
    for n in range(8):
        cols = slice(256 * n, 256 * n + 256)
        top_half = h0[:, cols].astype(f32) * tile(i0[...], 2) * gain[:, cols]
        low_half = h1[:, cols].astype(f32) * tile(i1[...], 2) * gain[:, cols]
        normed = jnp.concatenate([top_half.astype(bf16), low_half.astype(bf16)], axis=0)
        part = lax.dot_general(normed, vg[...], (((0,), (0,)), ((), ())), preferred_element_type=f32)
        part = part * scale
        for b in range(2):
            block = 2 * n + b
            row = pl.multiple_of(((((block % 4) ^ y) * 4) + ((block // 4) ^ low)) * 32, 32)
            for q in range(4):
                out[q ^ x, pl.ds(row, 32), :] = part[128 * b + 32 * q : 128 * b + 32 * q + 32, :]


def join_kernel(*refs):
    for at, r in enumerate(refs[:-1]):
        refs[-1][128 * at : 128 * at + 128, :] = r[0:128, :]


def grad_kernel(pos, *refs):
    y, z, low = pos[1], pos[2], pos[3]
    (own, a1, a2, a3, near, b1, b2, b3, far, c1, c2, c3, v0, v1, u0, u1, h0, h1, i0, i1, gain) = refs[:21]
    scaled, center, gain_sum, wide, vg = refs[21:]

    def place(value, dy, dz):
        there = lax.rem(z + dz + 8, 8)
        row = pl.multiple_of((lax.rem(there, 4) * 4 + (y ^ dy)) * 128, 128)
        wide[there // 4, pl.ds(row, 128), :] = value

    for dy, (o, n, f) in enumerate(((own, near, far), (a1, b1, c1), (a2, b2, c2), (a3, b3, c3))):
        place(o[...], dy, 0)
        for i, dz in enumerate((-1, 1, -2, 2)):
            place(n[128 * i : 128 * i + 128, :], dy, dz)
        for i, dz in enumerate((-3, 3, 4)):
            place(f[128 * i : 128 * i + 128, :], dy, dz)
    high = z // 4
    for at, top, bottom in ((high, v0, v1), (1 - high, u0, u1)):
        vg[at, 0:256, :] = top[...]
        vg[at, 256:512, :] = bottom[...]

    total = [jnp.zeros((256, 128), f32), jnp.zeros((256, 128), f32)]
    for n in range(8):
        cols = slice(256 * n, 256 * n + 256)
        gain_part = jnp.zeros((1, 256), f32)
        for t, (h, i) in enumerate(((h0, i0), (h1, i1))):
            rows = slice(256 * t, 256 * t + 256)
            grad = lax.dot_general(vg[0, rows, :], wide[0, cols, :], (((1,), (1,)), ((), ())), preferred_element_type=f32)
            grad += lax.dot_general(vg[1, rows, :], wide[1, cols, :], (((1,), (1,)), ((), ())), preferred_element_type=f32)
            normal = h[:, cols].astype(f32) * tile(i[...], 2)
            gain_part += jnp.sum(grad * normal, axis=0, keepdims=True)
            by_gain = grad * gain[:, cols]
            scaled[rows, cols] = by_gain
            product = by_gain * normal
            total[t] += product[:, :128] + product[:, 128:]
        for b in range(2):
            block = 2 * n + b
            row = ((block % 4) ^ y) * 4 + ((block // 4) ^ low)
            gain_sum[pl.ds(row, 1), :] = gain_part[:, 128 * b : 128 * b + 128]
    for t in range(2):
        center[256 * t : 256 * t + 256, :] = jnp.broadcast_to(jnp.sum(total[t], axis=1, keepdims=True), (256, 128))


def input_kernel(scaled, c_here, c_there, h0, h1, i0, i1, mine, other):
    for t, (h, i, out) in enumerate(((h0, i0, mine), (h1, i1, other))):
        rows, across = slice(256 * t, 256 * t + 256), slice(256 - 256 * t, 512 - 256 * t)
        center = (c_here[rows, :] + c_there[across, :]) * (1.0 / 4096)
        inv = i[...]
        for j in range(16):
            cols = slice(128 * j, 128 * j + 128)
            normal = h[:, cols].astype(f32) * inv
            out[:, cols] = (inv * (scaled[rows, cols] - normal * center)).astype(bf16)


def merge_kernel(pos, mine, other, out):
    core = pos[0]
    for j in range(16):
        cols = slice(128 * j, 128 * j + 128)
        a, b = mine[:, cols], other[:, cols]
        out[:, 256 * j : 256 * j + 128] = jnp.where(core == 0, a, b)
        out[:, 256 * j + 128 : 256 * j + 256] = jnp.where(core == 0, b, a)


def tree(a, b, c, d):
    return (a + b) + (c + d)


def low_kernel(total, g0, g1, g2, g3, *outs):
    for k, out in enumerate(outs):
        out[0:32, :] = total[32 * k : 32 * k + 32, :]
        out[32:40, :] = jnp.zeros((8, 512), f32)
        out[32:33, 0:128] = tree(*(g[4 * j + k : 4 * j + k + 1, :] for j, g in enumerate((g0, g1, g2, g3))))


def sum_kernel(a, b, c, d, out):
    out[...] = tree(a[...], b[...], c[...], d[...])


def place_kernel(pos, r0, r1, r2, r3, out, gain):
    refs = (r0, r1, r2, r3)
    for k, r in enumerate(refs):
        row = pl.multiple_of((pos[4] ^ k) * 32, 32)
        out[pl.ds(row, 32), :] = r[0:32, :]
    gain[...] = tree(*(r[32:33, 0:128] for r in refs)) * (1.0 / 128)


def local(hidden, norm_gain, value_weight, value_grad):
    x, fsdp, high = lax.axis_index("rep"), lax.axis_index("fsdp"), lax.axis_index("tp")
    core, y, low = fsdp % 2, (fsdp // 2) % 4, fsdp // 8
    pos = jnp.stack([core, y, high * 4 + low, low, x]).astype(jnp.int32)
    message = shape((8, 128))
    half = shape((256, 2048), bf16)

    own, v0, gain_row = value_weight, value_grad, norm_gain.reshape(1, 128)
    v1 = send(v0, core=1)
    a1, a3 = send(own, y=1), send(own, y=3)
    a2 = send(a1, y=3)
    ring = call(own_kernel, shape((144, 512), bf16), gain_row, own)
    m1, p1 = send(ring, z=1), send(ring, z=-1)
    m2, p2 = send(m1, z=1), send(p1, z=-1)
    m3, p3 = send(m2, z=1), send(p2, z=-1)
    q4 = send(m3, z=1)
    u0 = send(v0, z=4)
    u1 = send(u0, core=1)

    h0, give, i0 = call(split_kernel, (half, half, shape((256, 128))), pos, hidden, smem=1)
    h1, i1 = send(give, core=1), send(i0, core=1)
    second = call(second_kernel, message, pos, gain_row, m1, p1, m2, v0, v1, smem=1)
    gain, top = call(gain_kernel, (shape((1, 2048)), message), pos, second, *three([second] * 3, "y"), smem=1)

    near = call(join_kernel, shape((512, 512), bf16), m1, p1, m2, p2)
    b1, b3 = send(near, y=1), send(near, y=3)
    b2 = send(b1, y=3)
    far = call(join_kernel, shape((384, 512), bf16), m3, p3, q4)
    c1, c3 = send(far, y=1), send(far, y=3)
    c2 = send(c3, y=1)

    part = call(
        weight_kernel,
        shape((4, 512, 512)),
        pos, h0, h1, i0, i1, gain, top, v0, v1,
        smem=1,
        scratch=[pltpu.VMEM((512, 512), bf16)],
        flops=2 * 512 * 512 * 2048,
    )
    got = three([part[k].astype(f16) for k in (1, 2, 3)], "x")
    power = call(scale_kernel, shape((8, 512)), top, *three([top] * 3, "x"))
    total = tree(*(g.astype(f32) * power[k : k + 1] for k, g in enumerate([part[0], *got])))
    got = three([total[128 * k : 128 * k + 128].astype(f16) for k in (1, 2, 3)], "y")
    total = tree(total[:128], *(g.astype(f32) for g in got)) * power[4:5]
    scaled, center, gain_part = call(
        grad_kernel,
        (shape((512, 2048)), shape((512, 128)), shape((16, 128))),
        pos, own, a1, a2, a3, near, b1, b2, b3, far, c1, c2, c3, v0, v1, u0, u1, h0, h1, i0, i1, gain,
        smem=1,
        scratch=[pltpu.VMEM((2, 2048, 512), bf16), pltpu.VMEM((2, 512, 512), bf16)],
        flops=2 * 512 * 1024 * 2048,
    )
    across = send(center, core=1)
    mine, other = call(input_kernel, (half, half), scaled, center, across, h0, h1, i0, i1)
    input_grad = call(merge_kernel, shape((256, 4096), bf16), pos, mine, send(other, core=1), smem=1, last=True)

    row = shape((40, 512))
    lows = call(low_kernel, (row,) * 4, total, gain_part, *three([gain_part] * 3, "y"))
    final = call(sum_kernel, row, lows[0], *three(lows[1:], "low"))
    weight_grad, gain_grad = call(
        place_kernel,
        (shape((128, 512)), shape((1, 128))),
        pos, final, *three([final] * 3, "x"),
        smem=1,
        last=True,
    )
    return input_grad, weight_grad, gain_grad.reshape(128)


def solution(mesh):
    return jax.shard_map(
        local,
        mesh=mesh,
        in_specs=(P(("rep", "fsdp"), None), P("fsdp"), P("fsdp", "tp"), P(("rep", "fsdp"), "tp")),
        out_specs=(P(("rep", "fsdp"), None), P("fsdp", "tp"), P("fsdp")),
        check_vma=False,
    )
```

```python
import jax
import jax.numpy as jnp
from jax import lax
from jax.experimental import pallas as pl
from jax.experimental.pallas import tpu as pltpu
from jax.sharding import PartitionSpec as P

epsilon = 1e-05
AXES = ("rep", "fsdp", "tp")
LIMIT = 16 << 20
VMEM = pl.BlockSpec(memory_space=pltpu.VMEM)
SMEM = pl.BlockSpec(memory_space=pltpu.SMEM)
f32, bf16, f16 = jnp.float32, jnp.bfloat16, jnp.float16


def permutation(move):
    pairs = []
    for x in range(4):
        for low in range(4):
            for y in range(4):
                for core in range(2):
                    for high in range(2):
                        tx, ty, tz, tc = move(x, y, high * 4 + low, core)
                        source = (x * 32 + low * 8 + y * 2 + core) * 2 + high
                        target = (tx * 32 + (tz % 4) * 8 + ty * 2 + tc) * 2 + tz // 4
                        pairs.append((source, target))
    return pairs


def send(value, x=0, y=0, z=0, low=0, core=0, apart=0):
    def move(px, py, pz, pc):
        tz = (pz + z + (1 - 2 * pc) * apart) % 8
        return px ^ x, py ^ y, (tz // 4) * 4 + ((tz % 4) ^ low), pc ^ core

    return lax.ppermute(value, AXES, permutation(move))


def three(values, axis):
    return [send(values[k - 1], **{axis: k}) for k in (1, 2, 3)]


def call(kernel, out, *args, smem=0, scratch=(), flops=0, last=False):
    args = args[:smem] + tuple(pltpu.with_memory_space_constraint(a, pltpu.VMEM) for a in args[smem:])
    return pl.pallas_call(
        kernel,
        out_shape=out if last else jax.tree.map(lambda s: pltpu.VMEM(s.shape, s.dtype), out),
        in_specs=[SMEM] * smem + [VMEM] * (len(args) - smem),
        out_specs=jax.tree.map(lambda _: VMEM, out),
        scratch_shapes=scratch,
        compiler_params=pltpu.CompilerParams(vmem_limit_bytes=LIMIT),
        cost_estimate=pl.CostEstimate(flops=flops, bytes_accessed=1 << 22, transcendentals=0),
    )(*args)


def shape(dims, kind=f32):
    return jax.ShapeDtypeStruct(dims, kind)


def split_kernel(pos, h, mine, other, inv):
    core = pos[0]

    def rows(i, _):
        at = pl.ds(pl.multiple_of(i * 32, 32), 32)
        total = jnp.zeros((32, 128), f32)
        for j in range(16):
            even = h[at, 256 * j : 256 * j + 128]
            odd = h[at, 256 * j + 128 : 256 * j + 256]
            wide_even, wide_odd = even.astype(f32), odd.astype(f32)
            total += wide_even * wide_even + wide_odd * wide_odd
            mine[at, 128 * j : 128 * j + 128] = jnp.where(core == 0, even, odd)
            other[at, 128 * j : 128 * j + 128] = jnp.where(core == 0, odd, even)
        mean = jnp.sum(total, axis=1, keepdims=True) * (1.0 / 4096)
        inv[at, :] = jnp.broadcast_to(lax.rsqrt(mean + epsilon), (32, 128))
        return 0

    lax.fori_loop(0, 8, rows, 0)


def over(rows):
    a, b, c, d = rows
    return jnp.maximum(jnp.maximum(a, b), jnp.maximum(c, d))


def own_kernel(gain, own, ring):
    ring[0:128, :] = own[...]
    g = gain[...]
    top = g.astype(bf16)
    rest = g - top.astype(f32)
    middle = rest.astype(bf16)
    low = (rest - middle.astype(f32)).astype(bf16)
    line = jnp.concatenate([top, middle, low, low], axis=1)
    ring[128:144, :] = jnp.broadcast_to(line, (16, 512))


def second_kernel(pos, gain, m1, p1, m2, v0, v1, out):
    low = pos[3]
    out[pl.ds(low, 1), :] = gain[...]
    for dz, r in ((3, m1), (1, p1), (2, m2)):
        line = r[128:144, :].astype(f32)
        out[pl.ds((low + dz) & 3, 1), :] = (line[0:1, 0:128] + line[0:1, 128:256]) + line[0:1, 256:384]
    peak = jnp.maximum(jnp.max(jnp.abs(v0[...].astype(f32))), jnp.max(jnp.abs(v1[...].astype(f32))))
    out[4:8, :] = jnp.full((4, 128), peak, f32)


def gain_kernel(pos, r0, r1, r2, r3, out, top):
    y = pos[1]
    refs = (r0, r1, r2, r3)
    for b, r in enumerate(refs):
        for low in range(4):
            out[:, pl.ds(pl.multiple_of((low * 4 + (y ^ b)) * 128, 128), 128)] = r[low : low + 1, :]
    top[0:4, :] = r0[4:8, :]
    top[4:8, :] = over([r[4:8, :] for r in refs])


def exponent(top):
    return jnp.ceil(jnp.log2(jnp.maximum(top, 1e-30)))


def scale_kernel(t0, t1, t2, t3, power):
    refs = (t0, t1, t2, t3)
    wide = exponent(over([r[4:5, :] for r in refs])) + 2.0
    for k, r in enumerate(refs):
        power[k : k + 1, :] = tile(jnp.exp2(exponent(r[0:1, :]) - wide), 4)
    power[4:8, :] = jnp.broadcast_to(tile(jnp.exp2(wide) * (1.0 / 128), 4), (4, 512))


def tile(a, n):
    return jnp.concatenate([a] * n, axis=1)


def weight_kernel(pos, h0, h1, i0, i1, gain, top, v0, v1, out, vg):
    x, y, low = pos[4], pos[1], pos[3]
    vg[0:256, :] = v0[...]
    vg[256:512, :] = v1[...]
    scale = jnp.exp2(-exponent(top[0:1, :]))[0:1, 0:1]
    for n in range(8):
        cols = slice(256 * n, 256 * n + 256)
        top_half = h0[:, cols].astype(f32) * tile(i0[...], 2) * gain[:, cols]
        low_half = h1[:, cols].astype(f32) * tile(i1[...], 2) * gain[:, cols]
        normed = jnp.concatenate([top_half.astype(bf16), low_half.astype(bf16)], axis=0)
        part = lax.dot_general(normed, vg[...], (((0,), (0,)), ((), ())), preferred_element_type=f32)
        part = part * scale
        for b in range(2):
            block = 2 * n + b
            row = pl.multiple_of(((((block % 4) ^ y) * 4) + ((block // 4) ^ low)) * 32, 32)
            for q in range(4):
                out[q ^ x, pl.ds(row, 32), :] = part[128 * b + 32 * q : 128 * b + 32 * q + 32, :]


def join_kernel(*refs):
    for at, r in enumerate(refs[:-1]):
        refs[-1][128 * at : 128 * at + 128, :] = r[0:128, :]


def grad_kernel(pos, *refs):
    y, z, low = pos[1], pos[2], pos[3]
    (near, b1, b2, b3, far, c1, c2, c3, v0, v1, u0, u1, h0, h1, i0, i1, gain) = refs[:17]
    scaled, center, gain_sum, wide, vg = refs[17:]

    def place(value, dy, dz):
        there = lax.rem(z + dz + 8, 8)
        row = pl.multiple_of((lax.rem(there, 4) * 4 + (y ^ dy)) * 128, 128)
        wide[there // 4, pl.ds(row, 128), :] = value

    for dy, (n, f) in enumerate(((near, far), (b1, c1), (b2, c2), (b3, c3))):
        for i, dz in enumerate((0, -1, 1, -2, 2)):
            place(n[128 * i : 128 * i + 128, :], dy, dz)
        for i, dz in enumerate((-3, 3, 4)):
            place(f[128 * i : 128 * i + 128, :], dy, dz)
    high = z // 4
    for at, top, bottom in ((high, v0, v1), (1 - high, u0, u1)):
        vg[at, 0:256, :] = top[...]
        vg[at, 256:512, :] = bottom[...]

    total = [jnp.zeros((256, 128), f32), jnp.zeros((256, 128), f32)]
    for n in range(8):
        cols = slice(256 * n, 256 * n + 256)
        gain_part = jnp.zeros((1, 256), f32)
        for t, (h, i) in enumerate(((h0, i0), (h1, i1))):
            rows = slice(256 * t, 256 * t + 256)
            grad = lax.dot_general(vg[0, rows, :], wide[0, cols, :], (((1,), (1,)), ((), ())), preferred_element_type=f32)
            grad += lax.dot_general(vg[1, rows, :], wide[1, cols, :], (((1,), (1,)), ((), ())), preferred_element_type=f32)
            normal = h[:, cols].astype(f32) * tile(i[...], 2)
            gain_part += jnp.sum(grad * normal, axis=0, keepdims=True)
            by_gain = grad * gain[:, cols]
            scaled[rows, cols] = by_gain
            product = by_gain * normal
            total[t] += product[:, :128] + product[:, 128:]
        for b in range(2):
            block = 2 * n + b
            row = ((block % 4) ^ y) * 4 + ((block // 4) ^ low)
            gain_sum[pl.ds(row, 1), :] = gain_part[:, 128 * b : 128 * b + 128]
    for t in range(2):
        center[256 * t : 256 * t + 256, :] = jnp.broadcast_to(jnp.sum(total[t], axis=1, keepdims=True), (256, 128))


def input_kernel(scaled, c_here, c_there, h0, h1, i0, i1, mine, other):
    for t, (h, i, out) in enumerate(((h0, i0, mine), (h1, i1, other))):
        rows, across = slice(256 * t, 256 * t + 256), slice(256 - 256 * t, 512 - 256 * t)
        center = (c_here[rows, :] + c_there[across, :]) * (1.0 / 4096)
        inv = i[...]
        for j in range(16):
            cols = slice(128 * j, 128 * j + 128)
            normal = h[:, cols].astype(f32) * inv
            out[:, cols] = (inv * (scaled[rows, cols] - normal * center)).astype(bf16)


def merge_kernel(pos, mine, other, out):
    core = pos[0]
    for j in range(16):
        cols = slice(128 * j, 128 * j + 128)
        a, b = mine[:, cols], other[:, cols]
        out[:, 256 * j : 256 * j + 128] = jnp.where(core == 0, a, b)
        out[:, 256 * j + 128 : 256 * j + 256] = jnp.where(core == 0, b, a)


def tree(a, b, c, d):
    return (a + b) + (c + d)


def low_kernel(total, g0, g1, g2, g3, *outs):
    for k, out in enumerate(outs):
        out[0:32, :] = total[32 * k : 32 * k + 32, :]
        out[32:40, :] = jnp.zeros((8, 512), f32)
        out[32:33, 0:128] = tree(*(g[4 * j + k : 4 * j + k + 1, :] for j, g in enumerate((g0, g1, g2, g3))))


def sum_kernel(a, b, c, d, out):
    out[...] = tree(a[...], b[...], c[...], d[...])


def place_kernel(pos, r0, r1, r2, r3, out, gain):
    refs = (r0, r1, r2, r3)
    for k, r in enumerate(refs):
        row = pl.multiple_of((pos[4] ^ k) * 32, 32)
        out[pl.ds(row, 32), :] = r[0:32, :]
    gain[...] = tree(*(r[32:33, 0:128] for r in refs)) * (1.0 / 128)


def local(hidden, norm_gain, value_weight, value_grad):
    x, fsdp, high = lax.axis_index("rep"), lax.axis_index("fsdp"), lax.axis_index("tp")
    core, y, low = fsdp % 2, (fsdp // 2) % 4, fsdp // 8
    pos = jnp.stack([core, y, high * 4 + low, low, x]).astype(jnp.int32)
    message = shape((8, 128))
    half = shape((256, 2048), bf16)

    own, v0, gain_row = value_weight, value_grad, norm_gain.reshape(1, 128)
    v1 = send(v0, core=1)
    ring = call(own_kernel, shape((144, 512), bf16), gain_row, own)
    m1, p1 = send(ring, z=1), send(ring, z=-1)
    m2, p2 = send(m1, z=1), send(p1, z=-1)
    m3, p3 = send(m2, z=1), send(p2, z=-1)
    q4 = send(m3, z=1)
    u0 = send(send(v0, apart=2), apart=2)
    u1 = send(u0, core=1)

    h0, give, i0 = call(split_kernel, (half, half, shape((256, 128))), pos, hidden, smem=1)
    h1, i1 = send(give, core=1), send(i0, core=1)
    second = call(second_kernel, message, pos, gain_row, m1, p1, m2, v0, v1, smem=1)
    gain, top = call(gain_kernel, (shape((1, 2048)), message), pos, second, *three([second] * 3, "y"), smem=1)

    near = call(join_kernel, shape((640, 512), bf16), own, m1, p1, m2, p2)
    b1, b3 = send(near, y=1), send(near, y=3)
    b2 = send(b1, y=3)
    far = call(join_kernel, shape((384, 512), bf16), m3, p3, q4)
    c1, c3 = send(far, y=1), send(far, y=3)
    c2 = send(c3, y=1)

    part = call(
        weight_kernel,
        shape((4, 512, 512)),
        pos, h0, h1, i0, i1, gain, top, v0, v1,
        smem=1,
        scratch=[pltpu.VMEM((512, 512), bf16)],
        flops=2 * 512 * 512 * 2048,
    )
    got = three([part[k].astype(f16) for k in (1, 2, 3)], "x")
    power = call(scale_kernel, shape((8, 512)), top, *three([top] * 3, "x"))
    total = tree(*(g.astype(f32) * power[k : k + 1] for k, g in enumerate([part[0], *got])))
    got = three([total[128 * k : 128 * k + 128].astype(f16) for k in (1, 2, 3)], "y")
    total = tree(total[:128], *(g.astype(f32) for g in got)) * power[4:5]
    scaled, center, gain_part = call(
        grad_kernel,
        (shape((512, 2048)), shape((512, 128)), shape((16, 128))),
        pos, near, b1, b2, b3, far, c1, c2, c3, v0, v1, u0, u1, h0, h1, i0, i1, gain,
        smem=1,
        scratch=[pltpu.VMEM((2, 2048, 512), bf16), pltpu.VMEM((2, 512, 512), bf16)],
        flops=2 * 512 * 1024 * 2048,
    )
    across = send(center, core=1)
    mine, other = call(input_kernel, (half, half), scaled, center, across, h0, h1, i0, i1)
    input_grad = call(merge_kernel, shape((256, 4096), bf16), pos, mine, send(other, core=1), smem=1, last=True)

    row = shape((40, 512))
    lows = call(low_kernel, (row,) * 4, total, gain_part, *three([gain_part] * 3, "y"))
    final = call(sum_kernel, row, lows[0], *three(lows[1:], "low"))
    weight_grad, gain_grad = call(
        place_kernel,
        (shape((128, 512)), shape((1, 128))),
        pos, final, *three([final] * 3, "x"),
        smem=1,
        last=True,
    )
    return input_grad, weight_grad, gain_grad.reshape(128)


def solution(mesh):
    return jax.shard_map(
        local,
        mesh=mesh,
        in_specs=(P(("rep", "fsdp"), None), P("fsdp"), P("fsdp", "tp"), P(("rep", "fsdp"), "tp")),
        out_specs=(P(("rep", "fsdp"), None), P("fsdp", "tp"), P("fsdp")),
        check_vma=False,
    )
```

```python
import jax
import jax.numpy as jnp
from jax import lax
from jax.experimental import pallas as pl
from jax.experimental.pallas import tpu as pltpu
from jax.sharding import PartitionSpec as P

epsilon = 1e-05
AXES = ("rep", "fsdp", "tp")
LIMIT = 16 << 20
VMEM = pl.BlockSpec(memory_space=pltpu.VMEM)
SMEM = pl.BlockSpec(memory_space=pltpu.SMEM)
f32, bf16, f16 = jnp.float32, jnp.bfloat16, jnp.float16


def permutation(move):
    pairs = []
    for x in range(4):
        for low in range(4):
            for y in range(4):
                for core in range(2):
                    for high in range(2):
                        tx, ty, tz, tc = move(x, y, high * 4 + low, core)
                        source = (x * 32 + low * 8 + y * 2 + core) * 2 + high
                        target = (tx * 32 + (tz % 4) * 8 + ty * 2 + tc) * 2 + tz // 4
                        pairs.append((source, target))
    return pairs


def send(value, x=0, y=0, z=0, low=0, core=0, apart=0):
    def move(px, py, pz, pc):
        tz = (pz + z + (1 - 2 * pc) * apart) % 8
        return px ^ x, py ^ y, (tz // 4) * 4 + ((tz % 4) ^ low), pc ^ core

    return lax.ppermute(value, AXES, permutation(move))


def three(values, axis):
    return [send(values[k - 1], **{axis: k}) for k in (1, 2, 3)]


def call(kernel, out, *args, smem=0, scratch=(), flops=0, last=False):
    args = args[:smem] + tuple(pltpu.with_memory_space_constraint(a, pltpu.VMEM) for a in args[smem:])
    return pl.pallas_call(
        kernel,
        out_shape=out if last else jax.tree.map(lambda s: pltpu.VMEM(s.shape, s.dtype), out),
        in_specs=[SMEM] * smem + [VMEM] * (len(args) - smem),
        out_specs=jax.tree.map(lambda _: VMEM, out),
        scratch_shapes=scratch,
        compiler_params=pltpu.CompilerParams(vmem_limit_bytes=LIMIT),
        cost_estimate=pl.CostEstimate(flops=flops, bytes_accessed=1 << 22, transcendentals=0),
    )(*args)


def shape(dims, kind=f32):
    return jax.ShapeDtypeStruct(dims, kind)


def split_kernel(pos, h, mine, other, inv):
    core = pos[0]

    def rows(i, _):
        at = pl.ds(pl.multiple_of(i * 32, 32), 32)
        total = jnp.zeros((32, 128), f32)
        for j in range(16):
            even = h[at, 256 * j : 256 * j + 128]
            odd = h[at, 256 * j + 128 : 256 * j + 256]
            wide_even, wide_odd = even.astype(f32), odd.astype(f32)
            total += wide_even * wide_even + wide_odd * wide_odd
            mine[at, 128 * j : 128 * j + 128] = jnp.where(core == 0, even, odd)
            other[at, 128 * j : 128 * j + 128] = jnp.where(core == 0, odd, even)
        mean = jnp.sum(total, axis=1, keepdims=True) * (1.0 / 4096)
        inv[at, :] = jnp.broadcast_to(lax.rsqrt(mean + epsilon), (32, 128))
        return 0

    lax.fori_loop(0, 8, rows, 0)


def over(rows):
    a, b, c, d = rows
    return jnp.maximum(jnp.maximum(a, b), jnp.maximum(c, d))


def own_kernel(gain, own, ring):
    ring[0:128, :] = own[...]
    g = gain[...]
    top = g.astype(bf16)
    rest = g - top.astype(f32)
    middle = rest.astype(bf16)
    low = (rest - middle.astype(f32)).astype(bf16)
    line = jnp.concatenate([top, middle, low, low], axis=1)
    ring[128:144, :] = jnp.broadcast_to(line, (16, 512))


def second_kernel(pos, gain, m1, p1, m2, v0, v1, out):
    low = pos[3]
    out[pl.ds(low, 1), :] = gain[...]
    for dz, r in ((3, m1), (1, p1), (2, m2)):
        line = r[128:144, :].astype(f32)
        out[pl.ds((low + dz) & 3, 1), :] = (line[0:1, 0:128] + line[0:1, 128:256]) + line[0:1, 256:384]
    peak = jnp.maximum(jnp.max(jnp.abs(v0[...].astype(f32))), jnp.max(jnp.abs(v1[...].astype(f32))))
    out[4:8, :] = jnp.full((4, 128), peak, f32)


def gain_kernel(pos, r0, r1, r2, r3, out, top):
    y = pos[1]
    refs = (r0, r1, r2, r3)
    for b, r in enumerate(refs):
        for low in range(4):
            out[:, pl.ds(pl.multiple_of((low * 4 + (y ^ b)) * 128, 128), 128)] = r[low : low + 1, :]
    top[0:4, :] = r0[4:8, :]
    top[4:8, :] = over([r[4:8, :] for r in refs])


def exponent(top):
    return jnp.ceil(jnp.log2(jnp.maximum(top, 1e-30)))


def scale_kernel(t0, t1, t2, t3, power):
    refs = (t0, t1, t2, t3)
    wide = exponent(over([r[4:5, :] for r in refs])) + 2.0
    for k, r in enumerate(refs):
        power[k : k + 1, :] = tile(jnp.exp2(exponent(r[0:1, :]) - wide), 4)
    power[4:8, :] = jnp.broadcast_to(tile(jnp.exp2(wide) * (1.0 / 128), 4), (4, 512))


def tile(a, n):
    return jnp.concatenate([a] * n, axis=1)


def weight_kernel(pos, h0, h1, i0, i1, gain, top, v0, v1, out, vg):
    x, y, low = pos[4], pos[1], pos[3]
    vg[0:256, :] = v0[...]
    vg[256:512, :] = v1[...]
    scale = jnp.exp2(-exponent(top[0:1, :]))[0:1, 0:1]
    for n in range(8):
        cols = slice(256 * n, 256 * n + 256)
        top_half = h0[:, cols].astype(f32) * tile(i0[...], 2) * gain[:, cols]
        low_half = h1[:, cols].astype(f32) * tile(i1[...], 2) * gain[:, cols]
        normed = jnp.concatenate([top_half.astype(bf16), low_half.astype(bf16)], axis=0)
        part = lax.dot_general(normed, vg[...], (((0,), (0,)), ((), ())), preferred_element_type=f32)
        part = part * scale
        for b in range(2):
            block = 2 * n + b
            row = pl.multiple_of(((((block % 4) ^ y) * 4) + ((block // 4) ^ low)) * 32, 32)
            for q in range(4):
                out[q ^ x, pl.ds(row, 32), :] = part[128 * b + 32 * q : 128 * b + 32 * q + 32, :]


def join_kernel(*refs):
    for at, r in enumerate(refs[:-1]):
        refs[-1][128 * at : 128 * at + 128, :] = r[0:128, :]


def grad_kernel(pos, *refs):
    y, z, low = pos[1], pos[2], pos[3]
    (own, a1, a2, a3, near, b1, b2, b3, far, c1, c2, c3, v0, v1, u0, u1, h0, h1, i0, i1, gain) = refs[:21]
    scaled, center, gain_sum, wide, vg = refs[21:]

    def place(value, dy, dz):
        there = lax.rem(z + dz + 8, 8)
        row = pl.multiple_of((lax.rem(there, 4) * 4 + (y ^ dy)) * 128, 128)
        wide[there // 4, pl.ds(row, 128), :] = value

    for dy, (o, n, f) in enumerate(((own, near, far), (a1, b1, c1), (a2, b2, c2), (a3, b3, c3))):
        place(o[...], dy, 0)
        for i, dz in enumerate((-1, 1, -2, 2)):
            place(n[128 * i : 128 * i + 128, :], dy, dz)
        for i, dz in enumerate((-3, 3, 4)):
            place(f[128 * i : 128 * i + 128, :], dy, dz)
    high = z // 4
    for at, top, bottom in ((high, v0, v1), (1 - high, u0, u1)):
        vg[at, 0:256, :] = top[...]
        vg[at, 256:512, :] = bottom[...]

    total = [jnp.zeros((256, 128), f32), jnp.zeros((256, 128), f32)]
    for n in range(8):
        cols = slice(256 * n, 256 * n + 256)
        gain_part = jnp.zeros((1, 256), f32)
        for t, (h, i) in enumerate(((h0, i0), (h1, i1))):
            rows = slice(256 * t, 256 * t + 256)
            grad = lax.dot_general(vg[0, rows, :], wide[0, cols, :], (((1,), (1,)), ((), ())), preferred_element_type=f32)
            grad += lax.dot_general(vg[1, rows, :], wide[1, cols, :], (((1,), (1,)), ((), ())), preferred_element_type=f32)
            normal = h[:, cols].astype(f32) * tile(i[...], 2)
            gain_part += jnp.sum(grad * normal, axis=0, keepdims=True)
            by_gain = grad * gain[:, cols]
            scaled[rows, cols] = by_gain
            product = by_gain * normal
            total[t] += product[:, :128] + product[:, 128:]
        for b in range(2):
            block = 2 * n + b
            row = ((block % 4) ^ y) * 4 + ((block // 4) ^ low)
            gain_sum[pl.ds(row, 1), :] = gain_part[:, 128 * b : 128 * b + 128]
    for t in range(2):
        center[256 * t : 256 * t + 256, :] = jnp.broadcast_to(jnp.sum(total[t], axis=1, keepdims=True), (256, 128))


def input_kernel(scaled, c_here, c_there, h0, h1, i0, i1, mine, other):
    for t, (h, i, out) in enumerate(((h0, i0, mine), (h1, i1, other))):
        rows, across = slice(256 * t, 256 * t + 256), slice(256 - 256 * t, 512 - 256 * t)
        center = (c_here[rows, :] + c_there[across, :]) * (1.0 / 4096)
        inv = i[...]
        for j in range(16):
            cols = slice(128 * j, 128 * j + 128)
            normal = h[:, cols].astype(f32) * inv
            out[:, cols] = (inv * (scaled[rows, cols] - normal * center)).astype(bf16)


def merge_kernel(pos, mine, other, out):
    core = pos[0]
    for j in range(16):
        cols = slice(128 * j, 128 * j + 128)
        a, b = mine[:, cols], other[:, cols]
        out[:, 256 * j : 256 * j + 128] = jnp.where(core == 0, a, b)
        out[:, 256 * j + 128 : 256 * j + 256] = jnp.where(core == 0, b, a)


def tree(a, b, c, d):
    return (a + b) + (c + d)


def low_kernel(total, g0, g1, g2, g3, *outs):
    for k, out in enumerate(outs):
        out[0:32, :] = total[32 * k : 32 * k + 32, :]
        out[32:40, :] = jnp.zeros((8, 512), f32)
        out[32:33, 0:128] = tree(*(g[4 * j + k : 4 * j + k + 1, :] for j, g in enumerate((g0, g1, g2, g3))))


def sum_kernel(a, b, c, d, out):
    out[...] = tree(a[...], b[...], c[...], d[...])


def place_kernel(pos, r0, r1, r2, r3, out, gain):
    refs = (r0, r1, r2, r3)
    for k, r in enumerate(refs):
        row = pl.multiple_of((pos[4] ^ k) * 32, 32)
        out[pl.ds(row, 32), :] = r[0:32, :]
    gain[...] = tree(*(r[32:33, 0:128] for r in refs)) * (1.0 / 128)


def local(hidden, norm_gain, value_weight, value_grad):
    x, fsdp, high = lax.axis_index("rep"), lax.axis_index("fsdp"), lax.axis_index("tp")
    core, y, low = fsdp % 2, (fsdp // 2) % 4, fsdp // 8
    pos = jnp.stack([core, y, high * 4 + low, low, x]).astype(jnp.int32)
    message = shape((8, 128))
    half = shape((256, 2048), bf16)

    own, v0, gain_row = value_weight, value_grad, norm_gain.reshape(1, 128)
    v1 = send(v0, core=1)
    ring = call(own_kernel, shape((144, 512), bf16), gain_row, own)
    m1, p1 = send(ring, z=1), send(ring, z=-1)
    a1, a3 = send(own, y=1), send(own, y=3)
    a2 = send(a3, y=1)
    m2, p2 = send(m1, z=1), send(p1, z=-1)
    m3, p3 = send(m2, z=1), send(p2, z=-1)
    q4 = send(m3, z=1)
    u0 = send(send(v0, apart=2), apart=2)
    u1 = send(u0, core=1)

    h0, give, i0 = call(split_kernel, (half, half, shape((256, 128))), pos, hidden, smem=1)
    h1, i1 = send(give, core=1), send(i0, core=1)
    second = call(second_kernel, message, pos, gain_row, m1, p1, m2, v0, v1, smem=1)
    gain, top = call(gain_kernel, (shape((1, 2048)), message), pos, second, *three([second] * 3, "y"), smem=1)

    near = call(join_kernel, shape((512, 512), bf16), m1, p1, m2, p2)
    b1, b3 = send(near, y=1), send(near, y=3)
    b2 = send(b1, y=3)
    far = call(join_kernel, shape((384, 512), bf16), m3, p3, q4)
    c1, c3 = send(far, y=1), send(far, y=3)
    c2 = send(c3, y=1)

    part = call(
        weight_kernel,
        shape((4, 512, 512)),
        pos, h0, h1, i0, i1, gain, top, v0, v1,
        smem=1,
        scratch=[pltpu.VMEM((512, 512), bf16)],
        flops=2 * 512 * 512 * 2048,
    )
    got = three([part[k].astype(f16) for k in (1, 2, 3)], "x")
    power = call(scale_kernel, shape((8, 512)), top, *three([top] * 3, "x"))
    total = tree(*(g.astype(f32) * power[k : k + 1] for k, g in enumerate([part[0], *got])))
    got = three([total[128 * k : 128 * k + 128].astype(f16) for k in (1, 2, 3)], "y")
    total = tree(total[:128], *(g.astype(f32) for g in got)) * power[4:5]
    scaled, center, gain_part = call(
        grad_kernel,
        (shape((512, 2048)), shape((512, 128)), shape((16, 128))),
        pos, own, a1, a2, a3, near, b1, b2, b3, far, c1, c2, c3, v0, v1, u0, u1, h0, h1, i0, i1, gain,
        smem=1,
        scratch=[pltpu.VMEM((2, 2048, 512), bf16), pltpu.VMEM((2, 512, 512), bf16)],
        flops=2 * 512 * 1024 * 2048,
    )
    across = send(center, core=1)
    mine, other = call(input_kernel, (half, half), scaled, center, across, h0, h1, i0, i1)
    input_grad = call(merge_kernel, shape((256, 4096), bf16), pos, mine, send(other, core=1), smem=1, last=True)

    row = shape((40, 512))
    lows = call(low_kernel, (row,) * 4, total, gain_part, *three([gain_part] * 3, "y"))
    final = call(sum_kernel, row, lows[0], *three(lows[1:], "low"))
    weight_grad, gain_grad = call(
        place_kernel,
        (shape((128, 512)), shape((1, 128))),
        pos, final, *three([final] * 3, "x"),
        smem=1,
        last=True,
    )
    return input_grad, weight_grad, gain_grad.reshape(128)


def solution(mesh):
    return jax.shard_map(
        local,
        mesh=mesh,
        in_specs=(P(("rep", "fsdp"), None), P("fsdp"), P("fsdp", "tp"), P(("rep", "fsdp"), "tp")),
        out_specs=(P(("rep", "fsdp"), None), P("fsdp", "tp"), P("fsdp")),
        check_vma=False,
    )
```

```python
import jax
import jax.numpy as jnp
from jax import lax
from jax.experimental import pallas as pl
from jax.experimental.pallas import tpu as pltpu
from jax.sharding import PartitionSpec as P

epsilon = 1e-05
AXES = ("rep", "fsdp", "tp")
LIMIT = 16 << 20
VMEM = pl.BlockSpec(memory_space=pltpu.VMEM)
SMEM = pl.BlockSpec(memory_space=pltpu.SMEM)
f32, bf16, f16 = jnp.float32, jnp.bfloat16, jnp.float16


def permutation(move):
    pairs = []
    for x in range(4):
        for low in range(4):
            for y in range(4):
                for core in range(2):
                    for high in range(2):
                        tx, ty, tz, tc = move(x, y, high * 4 + low, core)
                        source = (x * 32 + low * 8 + y * 2 + core) * 2 + high
                        target = (tx * 32 + (tz % 4) * 8 + ty * 2 + tc) * 2 + tz // 4
                        pairs.append((source, target))
    return pairs


def send(value, x=0, y=0, z=0, low=0, core=0, apart=0):
    def move(px, py, pz, pc):
        tz = (pz + z + (1 - 2 * pc) * apart) % 8
        return px ^ x, py ^ y, (tz // 4) * 4 + ((tz % 4) ^ low), pc ^ core

    return lax.ppermute(value, AXES, permutation(move))


def three(values, axis):
    return [send(values[k - 1], **{axis: k}) for k in (1, 2, 3)]


def call(kernel, out, *args, smem=0, scratch=(), flops=0, last=False):
    args = args[:smem] + tuple(pltpu.with_memory_space_constraint(a, pltpu.VMEM) for a in args[smem:])
    return pl.pallas_call(
        kernel,
        out_shape=out if last else jax.tree.map(lambda s: pltpu.VMEM(s.shape, s.dtype), out),
        in_specs=[SMEM] * smem + [VMEM] * (len(args) - smem),
        out_specs=jax.tree.map(lambda _: VMEM, out),
        scratch_shapes=scratch,
        compiler_params=pltpu.CompilerParams(vmem_limit_bytes=LIMIT),
        cost_estimate=pl.CostEstimate(flops=flops, bytes_accessed=1 << 22, transcendentals=0),
    )(*args)


def shape(dims, kind=f32):
    return jax.ShapeDtypeStruct(dims, kind)


def split_kernel(pos, h, mine, other, inv):
    core = pos[0]

    def rows(i, _):
        at = pl.ds(pl.multiple_of(i * 32, 32), 32)
        total = jnp.zeros((32, 128), f32)
        for j in range(16):
            even = h[at, 256 * j : 256 * j + 128]
            odd = h[at, 256 * j + 128 : 256 * j + 256]
            wide_even, wide_odd = even.astype(f32), odd.astype(f32)
            total += wide_even * wide_even + wide_odd * wide_odd
            mine[at, 128 * j : 128 * j + 128] = jnp.where(core == 0, even, odd)
            other[at, 128 * j : 128 * j + 128] = jnp.where(core == 0, odd, even)
        mean = jnp.sum(total, axis=1, keepdims=True) * (1.0 / 4096)
        inv[at, :] = jnp.broadcast_to(lax.rsqrt(mean + epsilon), (32, 128))
        return 0

    lax.fori_loop(0, 8, rows, 0)


def over(rows):
    a, b, c, d = rows
    return jnp.maximum(jnp.maximum(a, b), jnp.maximum(c, d))


def own_kernel(gain, own, ring):
    ring[0:128, :] = own[...]
    g = gain[...]
    top = g.astype(bf16)
    rest = g - top.astype(f32)
    middle = rest.astype(bf16)
    low = (rest - middle.astype(f32)).astype(bf16)
    line = jnp.concatenate([top, middle, low, low], axis=1)
    ring[128:144, :] = jnp.broadcast_to(line, (16, 512))


def second_kernel(pos, gain, m1, p1, m2, v0, v1, out):
    low = pos[3]
    out[pl.ds(low, 1), :] = gain[...]
    for dz, r in ((3, m1), (1, p1), (2, m2)):
        line = r[128:144, :].astype(f32)
        out[pl.ds((low + dz) & 3, 1), :] = (line[0:1, 0:128] + line[0:1, 128:256]) + line[0:1, 256:384]
    peak = jnp.maximum(jnp.max(jnp.abs(v0[...].astype(f32))), jnp.max(jnp.abs(v1[...].astype(f32))))
    out[4:8, :] = jnp.full((4, 128), peak, f32)


def gain_kernel(pos, r0, r1, r2, r3, out, top):
    y = pos[1]
    refs = (r0, r1, r2, r3)
    for b, r in enumerate(refs):
        for low in range(4):
            out[:, pl.ds(pl.multiple_of((low * 4 + (y ^ b)) * 128, 128), 128)] = r[low : low + 1, :]
    top[0:4, :] = r0[4:8, :]
    top[4:8, :] = over([r[4:8, :] for r in refs])


def exponent(top):
    return jnp.ceil(jnp.log2(jnp.maximum(top, 1e-30)))


def scale_kernel(t0, t1, t2, t3, power):
    refs = (t0, t1, t2, t3)
    wide = exponent(over([r[4:5, :] for r in refs])) + 2.0
    for k, r in enumerate(refs):
        power[k : k + 1, :] = tile(jnp.exp2(exponent(r[0:1, :]) - wide), 4)
    power[4:8, :] = jnp.broadcast_to(tile(jnp.exp2(wide) * (1.0 / 128), 4), (4, 512))


def tile(a, n):
    return jnp.concatenate([a] * n, axis=1)


def weight_kernel(pos, h0, h1, i0, i1, gain, top, v0, v1, out, vg):
    x, y, low = pos[4], pos[1], pos[3]
    vg[0:256, :] = v0[...]
    vg[256:512, :] = v1[...]
    scale = jnp.exp2(-exponent(top[0:1, :]))[0:1, 0:1]
    for n in range(8):
        cols = slice(256 * n, 256 * n + 256)
        top_half = h0[:, cols].astype(f32) * tile(i0[...], 2) * gain[:, cols]
        low_half = h1[:, cols].astype(f32) * tile(i1[...], 2) * gain[:, cols]
        normed = jnp.concatenate([top_half.astype(bf16), low_half.astype(bf16)], axis=0)
        part = lax.dot_general(normed, vg[...], (((0,), (0,)), ((), ())), preferred_element_type=f32)
        part = part * scale
        for b in range(2):
            block = 2 * n + b
            row = pl.multiple_of(((((block % 4) ^ y) * 4) + ((block // 4) ^ low)) * 32, 32)
            for q in range(4):
                out[q ^ x, pl.ds(row, 32), :] = part[128 * b + 32 * q : 128 * b + 32 * q + 32, :]


def join_kernel(*refs):
    for at, r in enumerate(refs[:-1]):
        refs[-1][128 * at : 128 * at + 128, :] = r[0:128, :]


def grad_kernel(pos, *refs):
    y, z, low = pos[1], pos[2], pos[3]
    (own, a1, a2, a3, near, b1, b2, b3, far, c1, c2, c3, v0, v1, u0, u1, h0, h1, i0, i1, gain) = refs[:21]
    scaled, center, gain_sum, wide, vg = refs[21:]

    def place(value, dy, dz):
        there = lax.rem(z + dz + 8, 8)
        row = pl.multiple_of((lax.rem(there, 4) * 4 + (y ^ dy)) * 128, 128)
        wide[there // 4, pl.ds(row, 128), :] = value

    for dy, (o, n, f) in enumerate(((own, near, far), (a1, b1, c1), (a2, b2, c2), (a3, b3, c3))):
        place(o[...], dy, 0)
        for i, dz in enumerate((-1, 1, -2, 2)):
            place(n[128 * i : 128 * i + 128, :], dy, dz)
        for i, dz in enumerate((-3, 3, 4)):
            place(f[128 * i : 128 * i + 128, :], dy, dz)
    high = z // 4
    for at, top, bottom in ((high, v0, v1), (1 - high, u0, u1)):
        vg[at, 0:256, :] = top[...]
        vg[at, 256:512, :] = bottom[...]

    total = [jnp.zeros((256, 128), f32), jnp.zeros((256, 128), f32)]
    for n in range(8):
        cols = slice(256 * n, 256 * n + 256)
        gain_part = jnp.zeros((1, 256), f32)
        for t, (h, i) in enumerate(((h0, i0), (h1, i1))):
            rows = slice(256 * t, 256 * t + 256)
            grad = lax.dot_general(vg[0, rows, :], wide[0, cols, :], (((1,), (1,)), ((), ())), preferred_element_type=f32)
            grad += lax.dot_general(vg[1, rows, :], wide[1, cols, :], (((1,), (1,)), ((), ())), preferred_element_type=f32)
            normal = h[:, cols].astype(f32) * tile(i[...], 2)
            gain_part += jnp.sum(grad * normal, axis=0, keepdims=True)
            by_gain = grad * gain[:, cols]
            scaled[rows, cols] = by_gain
            product = by_gain * normal
            total[t] += product[:, :128] + product[:, 128:]
        for b in range(2):
            block = 2 * n + b
            row = ((block % 4) ^ y) * 4 + ((block // 4) ^ low)
            gain_sum[pl.ds(row, 1), :] = gain_part[:, 128 * b : 128 * b + 128]
    for t in range(2):
        center[256 * t : 256 * t + 256, :] = jnp.broadcast_to(jnp.sum(total[t], axis=1, keepdims=True), (256, 128))


def input_kernel(scaled, c_here, c_there, h0, h1, i0, i1, mine, other):
    for t, (h, i, out) in enumerate(((h0, i0, mine), (h1, i1, other))):
        rows, across = slice(256 * t, 256 * t + 256), slice(256 - 256 * t, 512 - 256 * t)
        center = (c_here[rows, :] + c_there[across, :]) * (1.0 / 4096)
        inv = i[...]
        for j in range(16):
            cols = slice(128 * j, 128 * j + 128)
            normal = h[:, cols].astype(f32) * inv
            out[:, cols] = (inv * (scaled[rows, cols] - normal * center)).astype(bf16)


def merge_kernel(pos, mine, other, out):
    core = pos[0]
    for j in range(16):
        cols = slice(128 * j, 128 * j + 128)
        a, b = mine[:, cols], other[:, cols]
        out[:, 256 * j : 256 * j + 128] = jnp.where(core == 0, a, b)
        out[:, 256 * j + 128 : 256 * j + 256] = jnp.where(core == 0, b, a)


def tree(a, b, c, d):
    return (a + b) + (c + d)


def low_kernel(total, g0, g1, g2, g3, *outs):
    for k, out in enumerate(outs):
        for q in range(4):
            out[32 * q : 32 * q + 32, :] = total[32 * k : 32 * k + 32, 128 * q : 128 * q + 128]
        out[128:136, :] = jnp.zeros((8, 128), f32)
        out[128:129, :] = tree(*(g[4 * j + k : 4 * j + k + 1, :] for j, g in enumerate((g0, g1, g2, g3))))


def sum_kernel(a, b, c, d, out):
    out[...] = tree(a[...], b[...], c[...], d[...])


def place_kernel(pos, r0, r1, r2, r3, out, gain):
    refs = (r0, r1, r2, r3)
    for k, r in enumerate(refs):
        row = pl.multiple_of((pos[4] ^ k) * 32, 32)
        for q in range(4):
            out[pl.ds(row, 32), 128 * q : 128 * q + 128] = r[32 * q : 32 * q + 32, :]
    gain[...] = tree(*(r[128:129, :] for r in refs)) * (1.0 / 128)


def local(hidden, norm_gain, value_weight, value_grad):
    x, fsdp, high = lax.axis_index("rep"), lax.axis_index("fsdp"), lax.axis_index("tp")
    core, y, low = fsdp % 2, (fsdp // 2) % 4, fsdp // 8
    pos = jnp.stack([core, y, high * 4 + low, low, x]).astype(jnp.int32)
    message = shape((8, 128))
    half = shape((256, 2048), bf16)

    own, v0, gain_row = value_weight, value_grad, norm_gain.reshape(1, 128)
    v1 = send(v0, core=1)
    ring = call(own_kernel, shape((144, 512), bf16), gain_row, own)
    m1, p1 = send(ring, z=1), send(ring, z=-1)
    a1, a3 = send(own, y=1), send(own, y=3)
    a2 = send(a3, y=1)
    m2, p2 = send(m1, z=1), send(p1, z=-1)
    m3, p3 = send(m2, z=1), send(p2, z=-1)
    q4 = send(m3, z=1)
    u0 = send(send(v0, apart=2), apart=2)
    u1 = send(u0, core=1)

    h0, give, i0 = call(split_kernel, (half, half, shape((256, 128))), pos, hidden, smem=1)
    h1, i1 = send(give, core=1), send(i0, core=1)
    second = call(second_kernel, message, pos, gain_row, m1, p1, m2, v0, v1, smem=1)
    gain, top = call(gain_kernel, (shape((1, 2048)), message), pos, second, *three([second] * 3, "y"), smem=1)

    near = call(join_kernel, shape((512, 512), bf16), m1, p1, m2, p2)
    b1, b3 = send(near, y=1), send(near, y=3)
    b2 = send(b1, y=3)
    far = call(join_kernel, shape((384, 512), bf16), m3, p3, q4)
    c1, c3 = send(far, y=1), send(far, y=3)
    c2 = send(c3, y=1)

    part = call(
        weight_kernel,
        shape((4, 512, 512)),
        pos, h0, h1, i0, i1, gain, top, v0, v1,
        smem=1,
        scratch=[pltpu.VMEM((512, 512), bf16)],
        flops=2 * 512 * 512 * 2048,
    )
    got = three([part[k].astype(f16) for k in (1, 2, 3)], "x")
    power = call(scale_kernel, shape((8, 512)), top, *three([top] * 3, "x"))
    total = tree(*(g.astype(f32) * power[k : k + 1] for k, g in enumerate([part[0], *got])))
    got = three([total[128 * k : 128 * k + 128].astype(f16) for k in (1, 2, 3)], "y")
    total = tree(total[:128], *(g.astype(f32) for g in got)) * power[4:5]
    scaled, center, gain_part = call(
        grad_kernel,
        (shape((512, 2048)), shape((512, 128)), shape((16, 128))),
        pos, own, a1, a2, a3, near, b1, b2, b3, far, c1, c2, c3, v0, v1, u0, u1, h0, h1, i0, i1, gain,
        smem=1,
        scratch=[pltpu.VMEM((2, 2048, 512), bf16), pltpu.VMEM((2, 512, 512), bf16)],
        flops=2 * 512 * 1024 * 2048,
    )
    across = send(center, core=1)
    mine, other = call(input_kernel, (half, half), scaled, center, across, h0, h1, i0, i1)
    input_grad = call(merge_kernel, shape((256, 4096), bf16), pos, mine, send(other, core=1), smem=1, last=True)

    row = shape((136, 128))
    lows = call(low_kernel, (row,) * 4, total, gain_part, *three([gain_part] * 3, "y"))
    final = call(sum_kernel, row, lows[0], *three(lows[1:], "low"))
    weight_grad, gain_grad = call(
        place_kernel,
        (shape((128, 512)), shape((1, 128))),
        pos, final, *three([final] * 3, "x"),
        smem=1,
        last=True,
    )
    return input_grad, weight_grad, gain_grad.reshape(128)


def solution(mesh):
    return jax.shard_map(
        local,
        mesh=mesh,
        in_specs=(P(("rep", "fsdp"), None), P("fsdp"), P("fsdp", "tp"), P(("rep", "fsdp"), "tp")),
        out_specs=(P(("rep", "fsdp"), None), P("fsdp", "tp"), P("fsdp")),
        check_vma=False,
    )
```

```python
import jax
import jax.numpy as jnp
from jax import lax
from jax.experimental import pallas as pl
from jax.experimental.pallas import tpu as pltpu
from jax.sharding import PartitionSpec as P

epsilon = 1e-05
AXES = ("rep", "fsdp", "tp")
LIMIT = 16 << 20
VMEM = pl.BlockSpec(memory_space=pltpu.VMEM)
SMEM = pl.BlockSpec(memory_space=pltpu.SMEM)
HBM = pl.BlockSpec(memory_space=pltpu.HBM)
f32, bf16, f16 = jnp.float32, jnp.bfloat16, jnp.float16


def permutation(move):
    pairs = []
    for x in range(4):
        for low in range(4):
            for y in range(4):
                for core in range(2):
                    for high in range(2):
                        tx, ty, tz, tc = move(x, y, high * 4 + low, core)
                        source = (x * 32 + low * 8 + y * 2 + core) * 2 + high
                        target = (tx * 32 + (tz % 4) * 8 + ty * 2 + tc) * 2 + tz // 4
                        pairs.append((source, target))
    return pairs


def send(value, x=0, y=0, z=0, low=0, core=0, apart=0):
    def move(px, py, pz, pc):
        tz = (pz + z + (1 - 2 * pc) * apart) % 8
        return px ^ x, py ^ y, (tz // 4) * 4 + ((tz % 4) ^ low), pc ^ core

    return lax.ppermute(value, AXES, permutation(move))


def three(values, axis):
    return [send(values[k - 1], **{axis: k}) for k in (1, 2, 3)]


def call(kernel, out, *args, smem=0, hbm=0, scratch=(), flops=0, last=False):
    near = smem + hbm
    spaces = [pltpu.HBM] * hbm + [pltpu.VMEM] * (len(args) - near)
    args = args[:smem] + tuple(map(pltpu.with_memory_space_constraint, args[smem:], spaces))
    return pl.pallas_call(
        kernel,
        out_shape=out if last else jax.tree.map(lambda s: pltpu.VMEM(s.shape, s.dtype), out),
        in_specs=[SMEM] * smem + [HBM] * hbm + [VMEM] * (len(args) - near),
        out_specs=jax.tree.map(lambda _: VMEM, out),
        scratch_shapes=scratch,
        compiler_params=pltpu.CompilerParams(vmem_limit_bytes=LIMIT),
        cost_estimate=pl.CostEstimate(flops=flops, bytes_accessed=1 << 22, transcendentals=0),
    )(*args)


def shape(dims, kind=f32):
    return jax.ShapeDtypeStruct(dims, kind)


def split_kernel(pos, source, mine, other, inv, h, arrived):
    core = pos[0]
    pieces = [pl.ds(64 * i, 64) for i in range(4)]
    copies = [pltpu.make_async_copy(source.at[p], h.at[p], arrived.at[i]) for i, p in enumerate(pieces)]
    for copy in copies:
        copy.start()

    def rows(i, _):
        at = pl.ds(pl.multiple_of(i * 32, 32), 32)
        total = jnp.zeros((32, 128), f32)
        for j in range(16):
            even = h[at, 256 * j : 256 * j + 128]
            odd = h[at, 256 * j + 128 : 256 * j + 256]
            wide_even, wide_odd = even.astype(f32), odd.astype(f32)
            total += wide_even * wide_even + wide_odd * wide_odd
            mine[at, 128 * j : 128 * j + 128] = jnp.where(core == 0, even, odd)
            other[at, 128 * j : 128 * j + 128] = jnp.where(core == 0, odd, even)
        mean = jnp.sum(total, axis=1, keepdims=True) * (1.0 / 4096)
        inv[at, :] = jnp.broadcast_to(lax.rsqrt(mean + epsilon), (32, 128))
        return 0

    for i, copy in enumerate(copies):
        copy.wait()
        lax.fori_loop(2 * i, 2 * i + 2, rows, 0)


def over(rows):
    a, b, c, d = rows
    return jnp.maximum(jnp.maximum(a, b), jnp.maximum(c, d))


def own_kernel(gain, own, ring):
    ring[0:128, :] = own[...]
    g = gain[...]
    top = g.astype(bf16)
    rest = g - top.astype(f32)
    middle = rest.astype(bf16)
    low = (rest - middle.astype(f32)).astype(bf16)
    line = jnp.concatenate([top, middle, low, low], axis=1)
    ring[128:144, :] = jnp.broadcast_to(line, (16, 512))


def second_kernel(pos, gain, m1, p1, m2, v0, v1, out):
    low = pos[3]
    out[pl.ds(low, 1), :] = gain[...]
    for dz, r in ((3, m1), (1, p1), (2, m2)):
        line = r[128:144, :].astype(f32)
        out[pl.ds((low + dz) & 3, 1), :] = (line[0:1, 0:128] + line[0:1, 128:256]) + line[0:1, 256:384]
    peak = jnp.maximum(jnp.max(jnp.abs(v0[...].astype(f32))), jnp.max(jnp.abs(v1[...].astype(f32))))
    out[4:8, :] = jnp.full((4, 128), peak, f32)


def gain_kernel(pos, r0, r1, r2, r3, out, top):
    y = pos[1]
    refs = (r0, r1, r2, r3)
    for b, r in enumerate(refs):
        for low in range(4):
            out[:, pl.ds(pl.multiple_of((low * 4 + (y ^ b)) * 128, 128), 128)] = r[low : low + 1, :]
    top[0:4, :] = r0[4:8, :]
    top[4:8, :] = over([r[4:8, :] for r in refs])


def exponent(top):
    return jnp.ceil(jnp.log2(jnp.maximum(top, 1e-30)))


def scale_kernel(t0, t1, t2, t3, power):
    refs = (t0, t1, t2, t3)
    wide = exponent(over([r[4:5, :] for r in refs])) + 2.0
    for k, r in enumerate(refs):
        power[k : k + 1, :] = tile(jnp.exp2(exponent(r[0:1, :]) - wide), 4)
    power[4:8, :] = jnp.broadcast_to(tile(jnp.exp2(wide) * (1.0 / 128), 4), (4, 512))


def tile(a, n):
    return jnp.concatenate([a] * n, axis=1)


def weight_kernel(pos, h0, h1, i0, i1, gain, top, v0, v1, out, vg):
    x, y, low = pos[4], pos[1], pos[3]
    vg[0:256, :] = v0[...]
    vg[256:512, :] = v1[...]
    scale = jnp.exp2(-exponent(top[0:1, :]))[0:1, 0:1]
    for n in range(8):
        cols = slice(256 * n, 256 * n + 256)
        top_half = h0[:, cols].astype(f32) * tile(i0[...], 2) * gain[:, cols]
        low_half = h1[:, cols].astype(f32) * tile(i1[...], 2) * gain[:, cols]
        normed = jnp.concatenate([top_half.astype(bf16), low_half.astype(bf16)], axis=0)
        part = lax.dot_general(normed, vg[...], (((0,), (0,)), ((), ())), preferred_element_type=f32)
        part = part * scale
        for b in range(2):
            block = 2 * n + b
            row = pl.multiple_of(((((block % 4) ^ y) * 4) + ((block // 4) ^ low)) * 32, 32)
            for q in range(4):
                out[q ^ x, pl.ds(row, 32), :] = part[128 * b + 32 * q : 128 * b + 32 * q + 32, :]


def join_kernel(*refs):
    for at, r in enumerate(refs[:-1]):
        refs[-1][128 * at : 128 * at + 128, :] = r[0:128, :]


def grad_kernel(pos, *refs):
    y, z, low = pos[1], pos[2], pos[3]
    (own, a1, a2, a3, near, b1, b2, b3, far, c1, c2, c3, v0, v1, u0, u1, h0, h1, i0, i1, gain) = refs[:21]
    scaled, center, gain_sum, wide, vg = refs[21:]

    def place(value, dy, dz):
        there = lax.rem(z + dz + 8, 8)
        row = pl.multiple_of((lax.rem(there, 4) * 4 + (y ^ dy)) * 128, 128)
        wide[there // 4, pl.ds(row, 128), :] = value

    for dy, (o, n, f) in enumerate(((own, near, far), (a1, b1, c1), (a2, b2, c2), (a3, b3, c3))):
        place(o[...], dy, 0)
        for i, dz in enumerate((-1, 1, -2, 2)):
            place(n[128 * i : 128 * i + 128, :], dy, dz)
        for i, dz in enumerate((-3, 3, 4)):
            place(f[128 * i : 128 * i + 128, :], dy, dz)
    high = z // 4
    for at, top, bottom in ((high, v0, v1), (1 - high, u0, u1)):
        vg[at, 0:256, :] = top[...]
        vg[at, 256:512, :] = bottom[...]

    total = [jnp.zeros((256, 128), f32), jnp.zeros((256, 128), f32)]
    for n in range(8):
        cols = slice(256 * n, 256 * n + 256)
        gain_part = jnp.zeros((1, 256), f32)
        for t, (h, i) in enumerate(((h0, i0), (h1, i1))):
            rows = slice(256 * t, 256 * t + 256)
            grad = lax.dot_general(vg[0, rows, :], wide[0, cols, :], (((1,), (1,)), ((), ())), preferred_element_type=f32)
            grad += lax.dot_general(vg[1, rows, :], wide[1, cols, :], (((1,), (1,)), ((), ())), preferred_element_type=f32)
            normal = h[:, cols].astype(f32) * tile(i[...], 2)
            gain_part += jnp.sum(grad * normal, axis=0, keepdims=True)
            by_gain = grad * gain[:, cols]
            scaled[rows, cols] = by_gain
            product = by_gain * normal
            total[t] += product[:, :128] + product[:, 128:]
        for b in range(2):
            block = 2 * n + b
            row = ((block % 4) ^ y) * 4 + ((block // 4) ^ low)
            gain_sum[pl.ds(row, 1), :] = gain_part[:, 128 * b : 128 * b + 128]
    for t in range(2):
        center[256 * t : 256 * t + 256, :] = jnp.broadcast_to(jnp.sum(total[t], axis=1, keepdims=True), (256, 128))


def input_kernel(scaled, c_here, c_there, h0, h1, i0, i1, mine, other):
    for t, (h, i, out) in enumerate(((h0, i0, mine), (h1, i1, other))):
        rows, across = slice(256 * t, 256 * t + 256), slice(256 - 256 * t, 512 - 256 * t)
        center = (c_here[rows, :] + c_there[across, :]) * (1.0 / 4096)
        inv = i[...]
        for j in range(16):
            cols = slice(128 * j, 128 * j + 128)
            normal = h[:, cols].astype(f32) * inv
            out[:, cols] = (inv * (scaled[rows, cols] - normal * center)).astype(bf16)


def merge_kernel(pos, mine, other, out):
    core = pos[0]
    for j in range(16):
        cols = slice(128 * j, 128 * j + 128)
        a, b = mine[:, cols], other[:, cols]
        out[:, 256 * j : 256 * j + 128] = jnp.where(core == 0, a, b)
        out[:, 256 * j + 128 : 256 * j + 256] = jnp.where(core == 0, b, a)


def tree(a, b, c, d):
    return (a + b) + (c + d)


def low_kernel(total, g0, g1, g2, g3, *outs):
    for k, out in enumerate(outs):
        for q in range(4):
            out[32 * q : 32 * q + 32, :] = total[32 * k : 32 * k + 32, 128 * q : 128 * q + 128]
        out[128:136, :] = jnp.zeros((8, 128), f32)
        out[128:129, :] = tree(*(g[4 * j + k : 4 * j + k + 1, :] for j, g in enumerate((g0, g1, g2, g3))))


def sum_kernel(a, b, c, d, out):
    out[...] = tree(a[...], b[...], c[...], d[...])


def place_kernel(pos, r0, r1, r2, r3, out, gain):
    refs = (r0, r1, r2, r3)
    for k, r in enumerate(refs):
        row = pl.multiple_of((pos[4] ^ k) * 32, 32)
        for q in range(4):
            out[pl.ds(row, 32), 128 * q : 128 * q + 128] = r[32 * q : 32 * q + 32, :]
    gain[...] = tree(*(r[128:129, :] for r in refs)) * (1.0 / 128)


def local(hidden, norm_gain, value_weight, value_grad):
    x, fsdp, high = lax.axis_index("rep"), lax.axis_index("fsdp"), lax.axis_index("tp")
    core, y, low = fsdp % 2, (fsdp // 2) % 4, fsdp // 8
    pos = jnp.stack([core, y, high * 4 + low, low, x]).astype(jnp.int32)
    message = shape((8, 128))
    half = shape((256, 2048), bf16)

    own, v0, gain_row = value_weight, value_grad, norm_gain.reshape(1, 128)
    v1 = send(v0, core=1)
    ring = call(own_kernel, shape((144, 512), bf16), gain_row, own)
    m1, p1 = send(ring, z=1), send(ring, z=-1)
    a1, a3 = send(own, y=1), send(own, y=3)
    a2 = send(a3, y=1)
    m2, p2 = send(m1, z=1), send(p1, z=-1)
    m3, p3 = send(m2, z=1), send(p2, z=-1)
    q4 = send(m3, z=1)
    u0 = send(send(v0, apart=2), apart=2)
    u1 = send(u0, core=1)

    h0, give, i0 = call(
        split_kernel,
        (half, half, shape((256, 128))),
        pos, hidden,
        smem=1,
        hbm=1,
        scratch=[pltpu.VMEM((256, 4096), bf16), pltpu.SemaphoreType.DMA((4,))],
    )
    h1, i1 = send(give, core=1), send(i0, core=1)
    second = call(second_kernel, message, pos, gain_row, m1, p1, m2, v0, v1, smem=1)
    gain, top = call(gain_kernel, (shape((1, 2048)), message), pos, second, *three([second] * 3, "y"), smem=1)

    near = call(join_kernel, shape((512, 512), bf16), m1, p1, m2, p2)
    b1, b3 = send(near, y=1), send(near, y=3)
    b2 = send(b1, y=3)
    far = call(join_kernel, shape((384, 512), bf16), m3, p3, q4)
    c1, c3 = send(far, y=1), send(far, y=3)
    c2 = send(c3, y=1)

    part = call(
        weight_kernel,
        shape((4, 512, 512)),
        pos, h0, h1, i0, i1, gain, top, v0, v1,
        smem=1,
        scratch=[pltpu.VMEM((512, 512), bf16)],
        flops=2 * 512 * 512 * 2048,
    )
    got = three([part[k].astype(f16) for k in (1, 2, 3)], "x")
    power = call(scale_kernel, shape((8, 512)), top, *three([top] * 3, "x"))
    total = tree(*(g.astype(f32) * power[k : k + 1] for k, g in enumerate([part[0], *got])))
    got = three([total[128 * k : 128 * k + 128].astype(f16) for k in (1, 2, 3)], "y")
    total = tree(total[:128], *(g.astype(f32) for g in got)) * power[4:5]
    scaled, center, gain_part = call(
        grad_kernel,
        (shape((512, 2048)), shape((512, 128)), shape((16, 128))),
        pos, own, a1, a2, a3, near, b1, b2, b3, far, c1, c2, c3, v0, v1, u0, u1, h0, h1, i0, i1, gain,
        smem=1,
        scratch=[pltpu.VMEM((2, 2048, 512), bf16), pltpu.VMEM((2, 512, 512), bf16)],
        flops=2 * 512 * 1024 * 2048,
    )
    across = send(center, core=1)
    mine, other = call(input_kernel, (half, half), scaled, center, across, h0, h1, i0, i1)
    input_grad = call(merge_kernel, shape((256, 4096), bf16), pos, mine, send(other, core=1), smem=1, last=True)

    row = shape((136, 128))
    lows = call(low_kernel, (row,) * 4, total, gain_part, *three([gain_part] * 3, "y"))
    final = call(sum_kernel, row, lows[0], *three(lows[1:], "low"))
    weight_grad, gain_grad = call(
        place_kernel,
        (shape((128, 512)), shape((1, 128))),
        pos, final, *three([final] * 3, "x"),
        smem=1,
        last=True,
    )
    return input_grad, weight_grad, gain_grad.reshape(128)


def solution(mesh):
    return jax.shard_map(
        local,
        mesh=mesh,
        in_specs=(P(("rep", "fsdp"), None), P("fsdp"), P("fsdp", "tp"), P(("rep", "fsdp"), "tp")),
        out_specs=(P(("rep", "fsdp"), None), P("fsdp", "tp"), P("fsdp")),
        check_vma=False,
    )
```
